512 devices in a mesh: pool: 16 (over z, y_hi), fft: 32 (over x, y_lo, core).
Axes of the slice: x: 4, y: 8 (y_hi: 2, y_lo: 4; y = y_hi * 4 + y_lo), z: 8, core: 2. Of those that a mesh axis runs over, the one named last changes fastest.
Arguments:
- orbitals: bfloat16 [16, 2, 1, 160, 25600], P('pool', None, None, 'fft'), may hold values from -6 to 6
- stick_map: int32 [16000], replicated, may hold values from -1 to 25599, as said below
- kpoint_grid: int32 [16, 3], replicated, may hold values from 0 to 3, as said below
Outputs:
- exchange_action: bfloat16 [16, 2, 1, 160, 25600], P('pool', None, None, 'fft')
The draws below stay inside these ranges and needn't reach their ends.
Inputs may be any that keep to these rules, and one draw needn't show every extreme that they name: `stick_map`: entries other than -1 are distinct columns. Slots come in blocks of 500 per index of fft; in each block at least half of the slots are live, and in every draw some block has all 500 live. `kpoint_grid`: rows are distinct.
All inputs are finite; a program needn't handle non-finite values.
Results may differ from the reference program's by a relative error of at most 0.011.
Values may be sent and summed in bfloat16 or wider, within the bound.
A program may use at most 64 MiB of HBM per device.

```python
import math
import jax
import jax.numpy as jnp
from jax import lax

NG = 160
BANDS = 1
KMESH = 4
KPOINTS = 16
STICKS_DEV = 500
STICKS_ALL = 16000


def draw_stick_map(key, part):
    devices = STICKS_ALL // STICKS_DEV
    key_counts = jax.random.fold_in(key, 11)
    key_full = jax.random.fold_in(key, 12)
    key_order = jax.random.fold_in(key, 13)
    counts = jax.random.randint(key_counts, (devices,), STICKS_DEV // 2, STICKS_DEV + 1)
    full_device = jax.random.randint(key_full, (), 0, devices)
    device_ids = jnp.arange(devices, dtype=jnp.int32)
    counts = jnp.where(device_ids == full_device, STICKS_DEV, counts).astype(jnp.int32)
    offsets = jnp.cumsum(counts) - counts
    shuffled = jax.random.permutation(key_order, NG * NG).astype(jnp.int32)
    column_x = shuffled % NG
    column_y = shuffled // NG
    signed_x = jnp.where(column_x >= NG // 2, column_x - NG, column_x)
    signed_y = jnp.where(column_y >= NG // 2, column_y - NG, column_y)
    outside = (signed_x * signed_x + signed_y * signed_y > NG // 2 * (NG // 2)).astype(jnp.int32)
    ordering = jnp.argsort(outside, stable=True)
    columns = shuffled[ordering]
    slot_ids = jnp.arange(STICKS_DEV, dtype=jnp.int32)
    positions = offsets[:, None] + slot_ids[None, :]
    positions = jnp.minimum(positions, NG * NG - 1)
    chosen = columns[positions]
    filled = jnp.where(slot_ids[None, :] < counts[:, None], chosen, -1)
    return filled.reshape(STICKS_ALL).astype(jnp.int32)


def draw_kpoint_grid(key, part):
    picked = jax.random.permutation(jax.random.fold_in(key, 21), KMESH * KMESH * KMESH)[:KPOINTS].astype(jnp.int32)
    first = picked // (KMESH * KMESH)
    second = picked // KMESH % KMESH
    third = picked % KMESH
    return jnp.stack([first, second, third], axis=1).astype(jnp.int32)


def steps_of(key, extent, split, low, largest):
    def one(position, shards_of):
        heights = jax.random.uniform(jax.random.fold_in(jax.random.fold_in(key, 6), position), (shards_of,), jnp.float32, low / len(split), largest / len(split))
        return jnp.repeat(jnp.exp(heights), extent[position] // shards_of).reshape((-1,) + (1,) * (len(extent) - position - 1))

    level = one(*split[0])
    for cut in split[1:]:
        level = level * one(*cut)
    return level


def noise(stream_key, shape, spread, bound, cuts=(), kind=jnp.bfloat16):
    values = jax.random.normal(stream_key, shape, jnp.float32) * spread
    if len(cuts) > 0:
        values = steps_of(stream_key, shape, cuts, -0.22, 0.18) * values
    return jnp.clip(values, min=-bound, max=bound).astype(kind)


def setup_inputs(seed: int = 0) -> dict:
    seeds = jax.random.split(jax.random.key(seed), 4)
    return {
        "orbitals": noise(seeds[0], (KPOINTS, 2, BANDS, NG, NG * NG), 1.0, 6.0, ((0, 16), (3, 32))),
        "stick_map": draw_stick_map(jax.random.fold_in(seeds[3], 71), 0),
        "kpoint_grid": draw_kpoint_grid(jax.random.fold_in(seeds[3], 71), 0),
    }


SPACING_BOHR = 0.1875
SCREENING = 0.106


def dft_table(grid_size, orientation):
    positions = jnp.arange(grid_size, dtype=jnp.int32)
    product = (positions[:, None] * positions[None, :]) % grid_size
    angle = product.astype(jnp.float32) * (2.0 * math.pi / grid_size)
    cosine = jnp.cos(angle)
    sine = orientation * jnp.sin(angle)
    upper = jnp.stack([cosine, sine], axis=1)
    lower = jnp.stack([-sine, cosine], axis=1)
    return jnp.stack([upper, lower], axis=0).astype(jnp.bfloat16)


def signed(frequency, grid_size):
    return jnp.where(frequency >= grid_size // 2, frequency - grid_size, frequency)


def kernel_table(columns, shift_q, grid_size):
    live_slot = columns >= 0
    column_ids = jnp.where(live_slot, columns, 0)
    freq_x = signed(column_ids % grid_size, grid_size)
    freq_y = signed(column_ids // grid_size, grid_size)
    freq_z = signed(jnp.arange(grid_size, dtype=jnp.int32), grid_size)
    radius = grid_size // 2
    inside = (freq_x * freq_x + freq_y * freq_y)[None, :] + (freq_z * freq_z)[:, None] <= radius * radius
    inside = jnp.logical_and(inside, live_slot[None, :])
    wave_x = freq_x.astype(jnp.float32) + shift_q[0]
    wave_y = freq_y.astype(jnp.float32) + shift_q[1]
    wave_z = freq_z.astype(jnp.float32) + shift_q[2]
    square = (wave_z * wave_z)[:, None] + (wave_x * wave_x + wave_y * wave_y)[None, :]
    cell = SPACING_BOHR * grid_size
    exponent = (math.pi * math.pi) * square / (cell * cell * SCREENING * SCREENING)
    weights = (cell * cell / math.pi) * (-jnp.expm1(-exponent)) / square / (float(grid_size) ** 3)
    return jnp.where(inside, weights, 0.0).astype(jnp.float32)


def momentum(kpoint_grid, pool_rank, pool_count):
    pool_rows = jnp.arange(pool_count, dtype=jnp.int32)
    earlier = (pool_rank + pool_count - 1) % pool_count
    current = jnp.sum(jnp.where((pool_rows == pool_rank)[:, None], kpoint_grid, 0), axis=0)
    previous = jnp.sum(jnp.where((pool_rows == earlier)[:, None], kpoint_grid, 0), axis=0)
    return (current - previous).astype(jnp.float32) / KMESH


def pair_density(own_bands, received):
    band_count = own_bands.shape[1]
    real_own = own_bands[0].astype(jnp.float32)[:, None]
    imag_own = own_bands[1].astype(jnp.float32)[:, None]
    real_recv = received[0].astype(jnp.float32)[None]
    imag_recv = received[1].astype(jnp.float32)[None]
    real_part = real_recv * real_own + imag_recv * imag_own
    imag_part = real_recv * imag_own - imag_recv * real_own
    stacked = jnp.stack([real_part, imag_part], axis=2)
    return stacked.reshape((band_count * band_count, 2) + own_bands.shape[2:]).astype(jnp.bfloat16)


def action_of(received, field):
    band_count = received.shape[1]
    field = field.reshape((band_count, band_count) + field.shape[1:])
    real_recv = received[0].astype(jnp.float32)[None]
    imag_recv = received[1].astype(jnp.float32)[None]
    real_field = field[:, :, 0]
    imag_field = field[:, :, 1]
    real_part = -jnp.sum(real_recv * real_field - imag_recv * imag_field, axis=1)
    imag_part = -jnp.sum(real_recv * imag_field + imag_recv * real_field, axis=1)
    return jnp.stack([real_part, imag_part], axis=0).astype(jnp.bfloat16)


def apply_table(data, table, form):
    return jnp.einsum(form, data.astype(jnp.float32), table.astype(jnp.float32), precision=lax.Precision.HIGHEST)


def column_pass(picked, weights, forward, backward):
    spectrum = apply_table(picked, forward, "pczs,czdk->pdks")
    scaled = (spectrum * weights).astype(jnp.bfloat16)
    return apply_table(scaled, backward, "pczs,czdk->pdks").astype(jnp.bfloat16)


def reference(orbitals, stick_map, kpoint_grid):
    pool_count = orbitals.shape[0]
    grid_size = orbitals.shape[3]
    orbitals = orbitals.reshape(orbitals.shape[:4] + (grid_size, grid_size))
    forward = dft_table(grid_size, -1.0)
    backward = dft_table(grid_size, 1.0)
    live_slot = stick_map >= 0
    column_ids = jnp.where(live_slot, stick_map, 0).astype(jnp.int32)

    def one_pool(pool_rank):
        own_bands = lax.dynamic_index_in_dim(orbitals, pool_rank, 0, keepdims=False)
        earlier = ((pool_rank + pool_count - 1) % pool_count).astype(jnp.int32)
        received = lax.dynamic_index_in_dim(orbitals, earlier, 0, keepdims=False)
        density = pair_density(own_bands, received)
        along_x = apply_table(density, forward, "pczyx,cxek->pezyk").astype(jnp.bfloat16)
        along_y = apply_table(along_x, forward, "pczyx,cyek->pezkx").astype(jnp.bfloat16)
        flattened = along_y.reshape(along_y.shape[:3] + (grid_size * grid_size,))
        picked = jnp.where(live_slot, jnp.take(flattened, column_ids, axis=3), 0).astype(jnp.bfloat16)
        weights = kernel_table(stick_map, momentum(kpoint_grid, pool_rank, pool_count), grid_size)
        returned = column_pass(picked, weights, forward, backward)
        merged = jnp.zeros_like(flattened).at[:, :, :, column_ids].add(jnp.where(live_slot, returned, 0).astype(jnp.bfloat16))
        back_y = apply_table(merged.reshape(along_y.shape), backward, "pczkx,ckey->pezyx").astype(jnp.bfloat16)
        field = apply_table(back_y, backward, "pczyk,ckex->pezyx")
        result = action_of(received, field)
        return result.reshape(result.shape[:3] + (grid_size * grid_size,))

    return lax.map(one_pool, jnp.arange(pool_count, dtype=jnp.int32))
```

```python
import math

import jax
import jax.numpy as jnp
from jax import lax
from jax.sharding import PartitionSpec as P

NG = 160
KMESH = 4


SPACING_BOHR = 0.1875
SCREENING = 0.106


def shifted(value, axis, steps):
    count = lax.axis_size(axis)
    pairs = [(source, (source + steps) % count) for source in range(count)]
    return lax.ppermute(value, axis, pairs)


def dft_table(grid_size, orientation):
    positions = jnp.arange(grid_size, dtype=jnp.int32)
    product = positions[:, None] * positions[None, :] % grid_size
    angle = product.astype(jnp.float32) * (2.0 * math.pi / grid_size)
    cosine = jnp.cos(angle)
    sine = orientation * jnp.sin(angle)
    upper = jnp.stack([cosine, sine], axis=1)
    lower = jnp.stack([-sine, cosine], axis=1)
    return jnp.stack([upper, lower], axis=0).astype(jnp.bfloat16)


def signed(frequency, grid_size):
    return jnp.where(frequency >= grid_size // 2, frequency - grid_size, frequency)


def kernel_table(columns, shift_q, grid_size):
    live_slot = columns >= 0
    column_ids = jnp.where(live_slot, columns, 0)
    freq_x = signed(column_ids % grid_size, grid_size)
    freq_y = signed(column_ids // grid_size, grid_size)
    freq_z = signed(jnp.arange(grid_size, dtype=jnp.int32), grid_size)
    radius = grid_size // 2
    inside = (freq_x * freq_x + freq_y * freq_y)[None, :] + (freq_z * freq_z)[
        :, None
    ] <= radius * radius
    inside = jnp.logical_and(inside, live_slot[None, :])
    wave_x = freq_x.astype(jnp.float32) + shift_q[0]
    wave_y = freq_y.astype(jnp.float32) + shift_q[1]
    wave_z = freq_z.astype(jnp.float32) + shift_q[2]
    square = (wave_z * wave_z)[:, None] + (wave_x * wave_x + wave_y * wave_y)[None, :]
    cell = SPACING_BOHR * grid_size
    exponent = math.pi * math.pi * square / (cell * cell * SCREENING * SCREENING)
    weights = cell * cell / math.pi * -jnp.expm1(-exponent) / square / float(grid_size) ** 3
    return jnp.where(inside, weights, 0.0)


def momentum(kpoint_grid, pool_rank, pool_count):
    pool_rows = jnp.arange(pool_count, dtype=jnp.int32)
    earlier = (pool_rank + pool_count - 1) % pool_count
    current = jnp.sum(jnp.where((pool_rows == pool_rank)[:, None], kpoint_grid, 0), axis=0)
    previous = jnp.sum(jnp.where((pool_rows == earlier)[:, None], kpoint_grid, 0), axis=0)
    return (current - previous).astype(jnp.float32) / KMESH


def pair_density(own_bands, received):
    band_count = own_bands.shape[1]
    real_own = own_bands[0].astype(jnp.float32)[:, None]
    imag_own = own_bands[1].astype(jnp.float32)[:, None]
    real_recv = received[0].astype(jnp.float32)[None]
    imag_recv = received[1].astype(jnp.float32)[None]
    real_part = real_recv * real_own + imag_recv * imag_own
    imag_part = real_recv * imag_own - imag_recv * real_own
    stacked = jnp.stack([real_part, imag_part], axis=2)
    return stacked.reshape((band_count * band_count, 2) + own_bands.shape[2:]).astype(jnp.bfloat16)


def action_of(received, field):
    band_count = received.shape[1]
    field = field.reshape((band_count, band_count) + field.shape[1:])
    real_recv = received[0].astype(jnp.float32)[None]
    imag_recv = received[1].astype(jnp.float32)[None]
    real_field = field[:, :, 0]
    imag_field = field[:, :, 1]
    real_part = -jnp.sum(real_recv * real_field - imag_recv * imag_field, axis=1)
    imag_part = -jnp.sum(real_recv * imag_field + imag_recv * real_field, axis=1)
    return jnp.stack([real_part, imag_part], axis=0).astype(jnp.bfloat16)


def apply_table(data, table, form):
    return jnp.einsum(form, data, table, preferred_element_type=jnp.float32)


def column_pass(picked, weights, forward, backward):
    spectrum = apply_table(picked, forward, "pczs,czdk->pdks")
    scaled = (spectrum * weights).astype(jnp.bfloat16)
    return apply_table(scaled, backward, "pczs,czdk->pdks").astype(jnp.bfloat16)


def local(orbitals, stick_map, kpoint_grid):
    grid_size = NG
    moved = shifted(orbitals, "pool", 1)
    own_bands = orbitals[0].reshape(orbitals.shape[1:4] + (grid_size, grid_size))
    received = moved[0].reshape(orbitals.shape[1:4] + (grid_size, grid_size))
    fft_count = lax.axis_size("fft")
    fft_rank = lax.axis_index("fft")
    pool_count = lax.axis_size("pool")
    pool_rank = lax.axis_index("pool")
    shift_q = momentum(kpoint_grid, pool_rank, pool_count)
    forward = dft_table(grid_size, -1.0)
    backward = dft_table(grid_size, 1.0)
    column_share = grid_size * grid_size // fft_count
    share_ids = fft_rank * column_share + jnp.arange(column_share, dtype=jnp.int32)
    own_rows = fft_rank * (grid_size // fft_count) + jnp.arange(grid_size // fft_count, dtype=jnp.int32)
    row_hit = (stick_map[None, :] // grid_size == own_rows[:, None]) & (stick_map >= 0)[None, :]
    every_column = jnp.arange(grid_size, dtype=jnp.int32)
    column_hit = stick_map[None, :] % grid_size == every_column[:, None]
    counts = jnp.einsum(
        "rs,cs->rc",
        row_hit.astype(jnp.bfloat16),
        column_hit.astype(jnp.bfloat16),
        preferred_element_type=jnp.float32,
    )
    own_present = counts.reshape(column_share) > 0.5
    weights = kernel_table(jnp.where(own_present, share_ids, -1), shift_q, grid_size)

    def potential(pair_block):
        along_x = apply_table(pair_block, forward, "pczyx,cxek->pezyk").astype(jnp.bfloat16)
        along_y = apply_table(along_x, forward, "pczyx,cyek->pezkx").astype(jnp.bfloat16)
        piece_block = lax.all_to_all(along_y, "fft", split_axis=3, concat_axis=2, tiled=True)
        flat_piece = piece_block.reshape(piece_block.shape[:3] + (column_share,))
        scaled_back = column_pass(flat_piece, weights, forward, backward).reshape(piece_block.shape)
        spectrum = lax.all_to_all(scaled_back, "fft", split_axis=2, concat_axis=3, tiled=True)
        back_y = apply_table(spectrum, backward, "pczkx,ckey->pezyx").astype(jnp.bfloat16)
        return apply_table(back_y, backward, "pczyk,ckex->pezyx")

    density = pair_density(own_bands, received)
    field = lax.map(lambda single_pair: potential(single_pair[None])[0], density)
    result = action_of(received, field)
    return result.reshape((1,) + result.shape[:3] + (grid_size * grid_size,))


def solution(mesh):
    return jax.shard_map(
        local,
        mesh=mesh,
        in_specs=(P("pool", None, None, "fft", None), P(), P()),
        out_specs=P("pool", None, None, "fft", None),
        check_vma=False,
    )
```

```python
import functools
import math

import jax
import jax.numpy as jnp
import ml_dtypes
import numpy as np
from jax import lax
from jax.experimental import pallas as pl
from jax.experimental.pallas import tpu as pltpu
from jax.sharding import PartitionSpec as P

NG = 160
KMESH = 4
SPACING_BOHR = 0.1875
SCREENING = 0.106

FFT = 32
POOL = 16
PLANES = NG // FFT
ROWS = NG // FFT
QUADS = 4
FOLD = 4
DEEP = NG // FOLD
WIDE = NG * FOLD
BLOCK = (ROWS + 1) * PLANES * 2
PITCH = 72
LANES = 128
STICK_ROWS = 125


def main_kx():
    lanes = np.arange(LANES)
    return np.where(lanes < 64, lanes, lanes + 32)


def edge_kx():
    return 64 + np.arange(LANES) % 32


def edge_ky():
    slots = np.arange(FFT * QUADS)
    return (slots - 64) % NG


def complex_table(inputs, outputs, orientation):
    product = (np.asarray(outputs)[:, None] * np.asarray(inputs)[None, :]) % NG
    angle = product.astype(np.float32) * np.float32(2.0 * math.pi / NG)
    cosine = np.cos(angle)
    sine = orientation * np.sin(angle)
    upper = np.stack([cosine, -sine], axis=1)
    lower = np.stack([sine, cosine], axis=1)
    return np.stack([upper, lower], axis=0).astype(np.float32)


def tables():
    folded = np.arange(NG)
    y_order = 4 * (folded % DEEP) + folded // DEEP
    grid = np.arange(NG)
    ky_main = np.arange(NG).reshape(FFT, ROWS).T.reshape(-1)
    ky_edge = edge_ky().reshape(FFT, QUADS).T.reshape(-1)
    z_order = np.arange(NG).reshape(FFT, PLANES).T.reshape(-1)

    x_main = complex_table(grid, main_kx(), -1.0)
    x_edge = complex_table(grid, edge_kx(), -1.0)
    x_all = np.stack([x_main, x_edge], axis=0)
    fx = x_all.transpose(3, 4, 0, 1, 2).reshape(2 * NG, 4 * LANES)

    def y_table(ky, n):
        full = complex_table(y_order, ky, -1.0)
        return full.reshape(2, n, FFT, 2, NG)

    fym = y_table(ky_main, ROWS).transpose(1, 0, 2, 3, 4).reshape(2 * NG, 2 * NG)
    fye = y_table(ky_edge, QUADS).transpose(0, 2, 1, 3, 4).reshape(2 * FFT, QUADS * 2 * NG)

    fz = complex_table(z_order, grid, -1.0).reshape(2, NG, 2, PLANES, FFT)
    fz = fz.transpose(0, 1, 3, 2, 4).reshape(2 * NG, 2 * NG)
    bz = complex_table(grid, z_order, 1.0).reshape(2, PLANES, FFT, 2, NG)
    bz = bz.transpose(1, 0, 2, 3, 4).reshape(2 * NG, 2 * NG)

    bym = complex_table(ky_main, y_order, 1.0).reshape(2, NG, 2, ROWS, FFT)
    bym = bym.transpose(0, 1, 3, 2, 4).reshape(2 * NG, 2 * NG)
    bye = complex_table(ky_edge, y_order, 1.0).reshape(2, NG, 2, QUADS, FFT)
    bye = bye.transpose(0, 1, 3, 2, 4).reshape(2 * NG, QUADS * 2 * FFT)

    back_main = complex_table(main_kx(), grid, 1.0)
    back_edge = complex_table(edge_kx(), grid, 1.0)
    back = np.stack([back_main, back_edge], axis=0)
    bx = back.transpose(0, 3, 4, 1, 2).reshape(4 * LANES, 2, NG)
    bx = np.pad(bx, ((0, 0), (0, 0), (0, 256 - NG))).reshape(4 * LANES, 512)
    made = (fx, fym, fye, fz, bz, bym, bye, bx)
    return [jnp.asarray(t.astype(ml_dtypes.bfloat16)) for t in made]


def signed(frequency):
    return jnp.where(frequency >= NG // 2, frequency - NG, frequency)


def dot(a, b):
    return jnp.dot(a, b, preferred_element_type=jnp.float32)


def kernel(
    kgrid, orb, stick, fx_h, fym_h, fye_h, fz_h, bz_h, bym_h, bye_h, bx_h,
    out,
    fx, fym, fye, fz, bz, bym, bye, bx,
    wx, wb, rec, t_main, t_edge, acc, weights, mask,
    send1, recv1, send2, recv2,
    table_sem, shift_send, shift_recv, a_send, a_recv, b_send, b_recv,
):
    pool = lax.axis_index("pool")
    me = lax.axis_index("fft")
    after = lax.rem(pool + 1, POOL)
    before = lax.rem(pool + POOL - 1, POOL)
    mesh_id = pl.DeviceIdType.MESH

    barrier = pltpu.get_barrier_semaphore()
    pl.semaphore_signal(barrier, inc=1, device_id=(after, me), device_id_type=mesh_id)
    pl.semaphore_signal(barrier, inc=1, device_id=(before, me), device_id_type=mesh_id)

    def greet(k, carry):
        peer = lax.rem(me + k, FFT)
        pl.semaphore_signal(barrier, inc=1, device_id=(pool, peer), device_id_type=mesh_id)
        return carry

    lax.fori_loop(1, FFT, greet, 0)
    pairs = ((fx_h, fx), (fym_h, fym), (fye_h, fye), (fz_h, fz), (bz_h, bz), (bym_h, bym), (bye_h, bye), (bx_h, bx))
    loads = [pltpu.make_async_copy(far, near, table_sem.at[i]) for i, (far, near) in enumerate(pairs)]
    for load in loads:
        load.start()
    pl.semaphore_wait(barrier, FFT + 1)

    def shift(z):
        return pltpu.make_async_remote_copy(
            src_ref=orb.at[:, z], dst_ref=rec.at[:, z],
            send_sem=shift_send.at[z], recv_sem=shift_recv.at[z],
            device_id=(after, me), device_id_type=mesh_id,
        )

    for z in range(PLANES):
        shift(z).start()

    row8 = lax.broadcasted_iota(jnp.int32, (16, LANES), 0)
    edge_row = me * QUADS + (row8 - 8) - 64
    edge_row = jnp.where(edge_row < 0, edge_row + NG, edge_row)
    own_ky = jnp.where(row8 < ROWS, me * ROWS + row8, jnp.where((row8 >= 8) & (row8 < 8 + QUADS), edge_row, -7))
    rank = lax.broadcasted_iota(jnp.int32, (2 * LANES, LANES), 0)
    kx_main = jnp.where(rank < 64, rank, rank + 32)
    kx_edge = 64 + lax.rem(rank, 32)
    every_kx = jnp.where(rank < LANES, kx_main, kx_edge)

    def count(i, total):
        slots = stick[pl.ds(i, 1), :]
        ky = jnp.where(slots >= 0, slots // NG, -9)
        kx = slots - (slots // NG) * NG
        hit_y = jnp.where(own_ky == ky, 1.0, 0.0).astype(jnp.bfloat16)
        hit_x = jnp.where(every_kx == kx, 1.0, 0.0).astype(jnp.bfloat16)
        return total + lax.dot_general(hit_y, hit_x, (((1,), (1,)), ((), ())), preferred_element_type=jnp.float32)

    mask[...] = lax.fori_loop(0, STICK_ROWS, count, jnp.zeros((16, 2 * LANES), jnp.float32))

    q = [(kgrid[pool, i] - kgrid[before, i]).astype(jnp.float32) / KMESH for i in range(3)]
    lane = lax.broadcasted_iota(jnp.int32, (NG, LANES), 1)
    freq_z = signed(lax.broadcasted_iota(jnp.int32, (NG, LANES), 0))
    wave_z = freq_z.astype(jnp.float32) + q[2]
    cell = SPACING_BOHR * NG
    quad = lax.broadcasted_iota(jnp.int32, (1, LANES), 1) // 32
    for r in range(ROWS + 1):
        if r < ROWS:
            freq_x = jnp.where(lane < 64, lane, lane - LANES)
            freq_y = jnp.full((NG, LANES), signed(me * ROWS + r), jnp.int32)
            held = mask[pl.ds(r, 1), pl.ds(0, LANES)]
        else:
            freq_x = signed(64 + lax.rem(lane, 32))
            freq_y = me * QUADS + lane // 32 - 64
            held = jnp.zeros((1, LANES), jnp.float32)
            for e in range(QUADS):
                held = jnp.where(quad == e, mask[pl.ds(8 + e, 1), pl.ds(LANES, LANES)], held)
        inside = freq_x * freq_x + freq_y * freq_y + freq_z * freq_z <= (NG // 2) * (NG // 2)
        wave_x = freq_x.astype(jnp.float32) + q[0]
        wave_y = freq_y.astype(jnp.float32) + q[1]
        square = wave_z * wave_z + (wave_x * wave_x + wave_y * wave_y)
        exponent = math.pi * math.pi * square / (cell * cell * SCREENING * SCREENING)
        weight = cell * cell / math.pi * (1.0 - jnp.exp(-exponent)) / square / float(NG) ** 3
        weights[r] = jnp.where(inside & (held > 0.5), weight, 0.0)

    for load in loads:
        load.wait()

    wx[...] = jnp.zeros_like(wx)
    row_i = lax.broadcasted_iota(jnp.int32, (256, 256), 0)
    col_i = lax.broadcasted_iota(jnp.int32, (256, 256), 1)
    for b in range(FOLD):
        for p in range(2):
            wx[b, pl.ds(256 * p + 32 * b, NG), :] = fx[pl.ds(NG * p, NG), :]
            move = jnp.where(col_i == row_i + 32 * b, 1.0, 0.0).astype(jnp.bfloat16)
            wb[b, :, pl.ds(256 * p, 256)] = dot(bx[:, pl.ds(256 * p, 256)], move).astype(jnp.bfloat16)

    lane_quad = lax.broadcasted_iota(jnp.int32, (2 * NG, LANES), 1) // 32

    def forward(z, carry):
        shift(z).wait_recv()
        own_re = orb[0, z].astype(jnp.float32)
        own_im = orb[1, z].astype(jnp.float32)
        rec_re = rec[0, z].astype(jnp.float32)
        rec_im = rec[1, z].astype(jnp.float32)
        den_re = (rec_re * own_re + rec_im * own_im).astype(jnp.bfloat16)
        den_im = (rec_re * own_im - rec_im * own_re).astype(jnp.bfloat16)
        for b in range(FOLD):
            window = slice(128 * b, 128 * b + 256)
            along = dot(den_re[:, window], wx[b, :256, :]) + dot(den_im[:, window], wx[b, 256:, :])
            for p in range(2):
                t_main[pl.ds(NG * p + DEEP * b, DEEP), :] = along[:, LANES * p : LANES * (p + 1)]
                t_edge[pl.ds(NG * p + DEEP * b, DEEP), :] = along[:, LANES * (2 + p) : LANES * (3 + p)]
        made = dot(fym[...], t_main[...].astype(jnp.bfloat16))
        side = t_edge[...]
        edge = jnp.zeros((2 * FFT, LANES), jnp.float32)
        for e in range(QUADS):
            part = jnp.where(lane_quad == e, side, 0.0).astype(jnp.bfloat16)
            edge = edge + dot(fye[:, 2 * NG * e : 2 * NG * (e + 1)], part)
        for r in range(ROWS + 1):
            for p in range(2):
                piece = made[(2 * r + p) * FFT : (2 * r + p + 1) * FFT] if r < ROWS else edge[p * FFT : (p + 1) * FFT]
                acc[pl.ds(10 * r + p + 2 * z, FFT, stride=PITCH), :] = piece
        return carry

    lax.fori_loop(0, PLANES, forward, 0)

    def exchange(send, recv, send_sem, recv_sem):
        send[...] = acc[...].reshape(FFT, PITCH, LANES)[:, :BLOCK].astype(jnp.bfloat16)

        def copy(k):
            peer = lax.rem(me + k, FFT)
            return pltpu.make_async_remote_copy(
                src_ref=send.at[peer], dst_ref=recv.at[me],
                send_sem=send_sem.at[peer], recv_sem=recv_sem.at[me],
                device_id=(pool, peer), device_id_type=mesh_id,
            )

        def start(k, carry):
            copy(k).start()
            return carry

        lax.fori_loop(1, FFT, start, 0)
        recv[me] = send[me]

        def finish(k, carry):
            peer = lax.rem(me + k, FFT)
            pltpu.make_async_remote_copy(
                src_ref=send.at[peer], dst_ref=recv.at[peer],
                send_sem=send_sem.at[peer], recv_sem=recv_sem.at[peer],
                device_id=(pool, peer), device_id_type=mesh_id,
            ).wait_recv()
            return carry

        lax.fori_loop(1, FFT, finish, 0)

        def spread(d, carry):
            acc[pl.ds(pl.multiple_of(d * PITCH, 8), BLOCK), :] = recv[d].astype(jnp.float32)
            return carry

        lax.fori_loop(0, FFT, spread, 0)
        return copy

    first = exchange(send1, recv1, a_send, a_recv)

    def columns(start):
        return acc[pl.ds(start, FFT, stride=PITCH), :]

    for r in range(ROWS + 1):
        field = jnp.concatenate([columns(10 * r + i) for i in range(2 * PLANES)], axis=0).astype(jnp.bfloat16)
        spectrum = dot(fz[...], field)
        weight = weights[r]
        scaled = jnp.concatenate([spectrum[:NG] * weight, spectrum[NG:] * weight], axis=0).astype(jnp.bfloat16)
        returned = dot(bz[...], scaled)
        for i in range(2 * PLANES):
            acc[pl.ds(10 * r + i, FFT, stride=PITCH), :] = returned[FFT * i : FFT * (i + 1)]

    second = exchange(send2, recv2, b_send, b_recv)

    def inverse(z, carry):
        main = jnp.concatenate([columns(10 * r + p + 2 * z) for r in range(ROWS) for p in range(2)], axis=0)
        edge = jnp.concatenate([columns(10 * ROWS + p + 2 * z) for p in range(2)], axis=0)
        quads = lane_quad[: 2 * FFT]
        edges = jnp.concatenate([jnp.where(quads == e, edge, 0.0) for e in range(QUADS)], axis=0)
        t_main[...] = dot(bym[...], main.astype(jnp.bfloat16))
        t_edge[...] = dot(bye[...], edges.astype(jnp.bfloat16))
        shares = []
        for b in range(FOLD):
            parts = [t[pl.ds(NG * p + DEEP * b, DEEP), :] for t in (t_main, t_edge) for p in range(2)]
            shares.append(dot(jnp.concatenate(parts, axis=1).astype(jnp.bfloat16), wb[b]))
        rec_re = rec[0, z].astype(jnp.float32)
        rec_im = rec[1, z].astype(jnp.float32)
        field = []
        for p in range(2):
            lo = [s[:, 256 * p : 256 * p + 128] for s in shares]
            hi = [s[:, 256 * p + 128 : 256 * p + 256] for s in shares]
            tiles = [lo[0]] + [hi[b] + lo[b + 1] for b in range(FOLD - 1)] + [hi[FOLD - 1]]
            field.append(jnp.concatenate(tiles, axis=1))
        out[0, z] = (rec_im * field[1] - rec_re * field[0]).astype(jnp.bfloat16)
        out[1, z] = (-(rec_re * field[1] + rec_im * field[0])).astype(jnp.bfloat16)
        return carry

    lax.fori_loop(0, PLANES, inverse, 0)

    for z in range(PLANES):
        shift(z).wait_send()

    def drain(k, carry):
        first(k).wait_send()
        second(k).wait_send()
        return carry

    lax.fori_loop(1, FFT, drain, 0)


def local(orbitals, stick_map, kpoint_grid):
    orb = orbitals.reshape(2, PLANES, DEEP, WIDE)
    stick = stick_map.reshape(STICK_ROWS, LANES)
    constants = tables()
    vmem = pl.BlockSpec(memory_space=pltpu.VMEM)
    anywhere = pl.BlockSpec(memory_space=pl.ANY)
    bf16 = jnp.bfloat16
    result = pl.pallas_call(
        kernel,
        name="exchange_step",
        out_shape=jax.ShapeDtypeStruct(orb.shape, bf16),
        in_specs=[pl.BlockSpec(memory_space=pltpu.SMEM), vmem, vmem] + [anywhere] * len(constants),
        out_specs=vmem,
        scratch_shapes=[pltpu.VMEM(t.shape, bf16) for t in constants]
        + [
            pltpu.VMEM((FOLD, 512, 512), bf16),
            pltpu.VMEM((FOLD, 512, 512), bf16),
            pltpu.VMEM(orb.shape, bf16),
            pltpu.VMEM((2 * NG, LANES), jnp.float32),
            pltpu.VMEM((2 * NG, LANES), jnp.float32),
            pltpu.VMEM((FFT * PITCH, LANES), jnp.float32),
            pltpu.VMEM((ROWS + 1, NG, LANES), jnp.float32),
            pltpu.VMEM((16, 2 * LANES), jnp.float32),
        ]
        + [pltpu.VMEM((FFT, BLOCK, LANES), bf16)] * 4
        + [
            pltpu.SemaphoreType.DMA((len(constants),)),
            pltpu.SemaphoreType.DMA((PLANES,)),
            pltpu.SemaphoreType.DMA((PLANES,)),
        ]
        + [pltpu.SemaphoreType.DMA((FFT,))] * 4,
        compiler_params=pltpu.CompilerParams(
            collective_id=0, has_side_effects=True, vmem_limit_bytes=48 * 1024 * 1024
        ),
    )(kpoint_grid, orb, stick, *constants)
    return result.reshape(1, 2, 1, PLANES, NG * NG)


def solution(mesh):
    return jax.shard_map(
        local,
        mesh=mesh,
        in_specs=(P("pool", None, None, "fft", None), P(), P()),
        out_specs=P("pool", None, None, "fft", None),
        check_vma=False,
    )
```

```python
import functools
import math

import jax
import jax.numpy as jnp
import ml_dtypes
import numpy as np
from jax import lax
from jax.experimental import pallas as pl
from jax.experimental.pallas import tpu as pltpu
from jax.sharding import PartitionSpec as P

NG = 160
KMESH = 4
SPACING_BOHR = 0.1875
SCREENING = 0.106

FFT = 32
POOL = 16
PLANES = NG // FFT
ROWS = NG // FFT
QUADS = 4
FOLD = 4
DEEP = NG // FOLD
WIDE = NG * FOLD
GROUPS = ROWS + 1
PIECE = GROUPS * 2
PITCH = 24
TILES = WIDE // 128
RAW = 2 * TILES * DEEP
OTHERS = FFT - 1
LANES = 128
STICK_ROWS = 125


def main_kx():
    lanes = np.arange(LANES)
    return np.where(lanes < 64, lanes, lanes + 32)


def edge_kx():
    return 64 + np.arange(LANES) % 32


def edge_ky():
    slots = np.arange(FFT * QUADS)
    return (slots - 64) % NG


def complex_table(inputs, outputs, orientation):
    product = (np.asarray(outputs)[:, None] * np.asarray(inputs)[None, :]) % NG
    angle = product.astype(np.float32) * np.float32(2.0 * math.pi / NG)
    cosine = np.cos(angle)
    sine = orientation * np.sin(angle)
    upper = np.stack([cosine, -sine], axis=1)
    lower = np.stack([sine, cosine], axis=1)
    return np.stack([upper, lower], axis=0).astype(np.float32)


def tables():
    folded = np.arange(NG)
    y_order = 4 * (folded % DEEP) + folded // DEEP
    grid = np.arange(NG)
    ky_main = np.arange(NG).reshape(FFT, ROWS).T.reshape(-1)
    ky_edge = edge_ky().reshape(FFT, QUADS).T.reshape(-1)
    z_order = np.arange(NG).reshape(FFT, PLANES).T.reshape(-1)

    x_main = complex_table(grid, main_kx(), -1.0)
    x_edge = complex_table(grid, edge_kx(), -1.0)
    x_all = np.stack([x_main, x_edge], axis=0)
    fx = x_all.transpose(3, 4, 0, 1, 2).reshape(2 * NG, 4 * LANES)

    def y_table(ky, n):
        full = complex_table(y_order, ky, -1.0)
        return full.reshape(2, n, FFT, 2, NG)

    fym = y_table(ky_main, ROWS).transpose(1, 0, 2, 3, 4).reshape(2 * NG, 2 * NG)
    fye = y_table(ky_edge, QUADS).transpose(0, 2, 1, 3, 4).reshape(2 * FFT, QUADS * 2 * NG)

    fz = complex_table(z_order, grid, -1.0).reshape(2, NG, 2, PLANES, FFT)
    fz = fz.transpose(0, 1, 3, 2, 4).reshape(2 * NG, 2 * NG)
    bz = complex_table(grid, z_order, 1.0).reshape(2, PLANES, FFT, 2, NG)
    bz = bz.transpose(1, 0, 2, 3, 4).reshape(2 * NG, 2 * NG)

    bym = complex_table(ky_main, y_order, 1.0).reshape(2, NG, 2, ROWS, FFT)
    bym = bym.transpose(0, 1, 3, 2, 4).reshape(2 * NG, 2 * NG)
    bye = complex_table(ky_edge, y_order, 1.0).reshape(2, NG, 2, QUADS, FFT)
    bye = bye.transpose(0, 1, 3, 2, 4).reshape(2 * NG, QUADS * 2 * FFT)

    back_main = complex_table(main_kx(), grid, 1.0)
    back_edge = complex_table(edge_kx(), grid, 1.0)
    back = np.stack([back_main, back_edge], axis=0)
    bx = back.transpose(0, 3, 4, 1, 2).reshape(4 * LANES, 2, NG)
    bx = np.pad(bx, ((0, 0), (0, 0), (0, 256 - NG))).reshape(4 * LANES, 512)
    made = (fx, fym, fye, fz, bz, bym, bye, bx)
    return [jnp.asarray(t.astype(ml_dtypes.bfloat16)) for t in made]


def signed(frequency):
    return jnp.where(frequency >= NG // 2, frequency - NG, frequency)


def dot(a, b):
    return jnp.dot(a, b, preferred_element_type=jnp.float32)


def kernel(
    kgrid_h, orb, stick_h, fx_h, fym_h, fye_h, fz_h, bz_h, bym_h, bye_h, bx_h,
    out,
    kgrid, own, stick, fx, fym, fye, fz, bz, bym, bye, bx,
    wx, wb, rec, flat_a, flat_b, t_main, t_edge, stage, acc, weights, scaled, mask,
    send1, recv1, send2, recv2,
    load_sem, shift_send, shift_recv, a_send, a_recv, b_send, b_recv,
):
    pool = lax.axis_index("pool")
    me = lax.axis_index("fft")
    after = lax.rem(pool + 1, POOL)
    before = lax.rem(pool + POOL - 1, POOL)
    mesh_id = pl.DeviceIdType.MESH

    barrier = pltpu.get_barrier_semaphore()
    pl.semaphore_signal(barrier, inc=1, device_id=(before, me), device_id_type=mesh_id)

    def greet(k, carry):
        peer = lax.rem(me + k, FFT)
        pl.semaphore_signal(barrier, inc=1, device_id=(pool, peer), device_id_type=mesh_id)
        return carry

    lax.fori_loop(1, FFT, greet, 0)
    pairs = (
        (stick_h, stick), (kgrid_h, kgrid), (orb, own), (fx_h, fx), (bx_h, bx), (fym_h, fym),
        (fye_h, fye), (fz_h, fz), (bz_h, bz), (bym_h, bym), (bye_h, bye),
    )
    loads = [pltpu.make_async_copy(far, near, load_sem.at[i]) for i, (far, near) in enumerate(pairs)]
    for load in loads:
        load.start()
    pl.semaphore_wait(barrier, FFT)

    def shift(z):
        return pltpu.make_async_remote_copy(
            src_ref=orb.at[z], dst_ref=rec.at[z],
            send_sem=shift_send.at[z], recv_sem=shift_recv.at[z],
            device_id=(after, me), device_id_type=mesh_id,
        )

    for z in range(PLANES):
        shift(z).start()
    for load in loads:
        load.wait()

    row16 = lax.broadcasted_iota(jnp.int32, (16, LANES), 0)
    edge_row = me * QUADS + (row16 - 8) - 64
    edge_row = jnp.where(edge_row < 0, edge_row + NG, edge_row)
    own_ky = jnp.where(row16 < ROWS, me * ROWS + row16, jnp.where((row16 >= 8) & (row16 < 8 + QUADS), edge_row, -7))
    rank = lax.broadcasted_iota(jnp.int32, (2 * LANES, LANES), 0)
    kx_main = jnp.where(rank < 64, rank, rank + 32)
    kx_edge = 64 + lax.rem(rank, 32)
    every_kx = jnp.where(rank < LANES, kx_main, kx_edge)

    def count(i, total):
        hits_y, hits_x = [], []
        for u in range(5):
            slots = stick[pl.ds(5 * i + u, 1), :]
            row = slots // NG
            ky = jnp.where(slots >= 0, row, -9)
            kx = slots - row * NG
            hits_y.append(jnp.where(own_ky == ky, 1.0, 0.0))
            hits_x.append(jnp.where(every_kx == kx, 1.0, 0.0))
        hit_y = jnp.concatenate(hits_y, axis=1).astype(jnp.bfloat16)
        hit_x = jnp.concatenate(hits_x, axis=1).astype(jnp.bfloat16)
        return total + lax.dot_general(hit_y, hit_x, (((1,), (1,)), ((), ())), preferred_element_type=jnp.float32)

    mask[...] = lax.fori_loop(0, STICK_ROWS // 5, count, jnp.zeros((16, 2 * LANES), jnp.float32))

    pools = lax.broadcasted_iota(jnp.int32, (3, POOL), 1)
    moved = jnp.where(pools == pool, kgrid[...], 0) - jnp.where(pools == before, kgrid[...], 0)
    q = jnp.sum(moved.astype(jnp.float32), axis=1, keepdims=True) / KMESH
    lane = lax.broadcasted_iota(jnp.int32, (NG, LANES), 1)
    freq_z = signed(lax.broadcasted_iota(jnp.int32, (NG, LANES), 0))
    wave_z = freq_z.astype(jnp.float32) + q[2:3]
    cell = SPACING_BOHR * NG
    quad = lax.broadcasted_iota(jnp.int32, (1, LANES), 1) // 32
    for r in range(GROUPS):
        if r < ROWS:
            freq_x = jnp.where(lane < 64, lane, lane - LANES)
            freq_y = jnp.full((NG, LANES), signed(me * ROWS + r), jnp.int32)
            held = mask[pl.ds(r, 1), pl.ds(0, LANES)]
        else:
            freq_x = signed(64 + lax.rem(lane, 32))
            freq_y = me * QUADS + lane // 32 - 64
            held = jnp.zeros((1, LANES), jnp.float32)
            for e in range(QUADS):
                held = jnp.where(quad == e, mask[pl.ds(8 + e, 1), pl.ds(LANES, LANES)], held)
        inside = freq_x * freq_x + freq_y * freq_y + freq_z * freq_z <= (NG // 2) * (NG // 2)
        wave_x = freq_x.astype(jnp.float32) + q[0:1]
        wave_y = freq_y.astype(jnp.float32) + q[1:2]
        square = wave_z * wave_z + (wave_x * wave_x + wave_y * wave_y)
        exponent = math.pi * math.pi * square / (cell * cell * SCREENING * SCREENING)
        weight = cell * cell / math.pi * (1.0 - jnp.exp(-exponent)) / square / float(NG) ** 3
        weights[:, pl.ds(LANES * r, LANES)] = jnp.where(inside & (held > 0.5), weight, 0.0)

    wx[...] = jnp.zeros_like(wx)
    row_i = lax.broadcasted_iota(jnp.int32, (256, 256), 0)
    col_i = lax.broadcasted_iota(jnp.int32, (256, 256), 1)
    for b in range(FOLD):
        move = jnp.where(col_i == row_i + 32 * b, 1.0, 0.0).astype(jnp.bfloat16)
        for p in range(2):
            wx[b, pl.ds(256 * p + 32 * b, NG), :] = fx[pl.ds(NG * p, NG), :]
            wb[b, :, pl.ds(256 * p, 256)] = dot(bx[:, pl.ds(256 * p, 256)], move).astype(jnp.bfloat16)

    lane_quad = lax.broadcasted_iota(jnp.int32, (2 * NG, LANES), 1) // 32

    def piece_to(z, peer, send, recv, send_sem, recv_sem):
        return pltpu.make_async_remote_copy(
            src_ref=send.at[z, peer], dst_ref=recv.at[z, me],
            send_sem=send_sem, recv_sem=recv_sem,
            device_id=(pool, peer), device_id_type=mesh_id,
        )

    def post(z, send, recv, send_sem, recv_sem):
        send[z] = stage[...].reshape(FFT, PITCH, LANES)[:, :PIECE].astype(jnp.bfloat16)
        recv[z, me] = send[z, me]

        def start(k, carry):
            piece_to(z, lax.rem(me + k, FFT), send, recv, send_sem, recv_sem).start()
            return carry

        lax.fori_loop(1, FFT, start, 0)

    def halves(source, t):
        return [source[pl.ds(2 * t + p, DEEP, stride=2 * TILES), :] for p in range(2)]

    def forward(z, carry):
        flat_a[...] = own[z].astype(jnp.float32)
        shift(z).wait_recv()
        flat_b[...] = rec[z].astype(jnp.float32)
        den_re, den_im = [], []
        for t in range(TILES):
            own_re, own_im = halves(flat_a, t)
            rec_re, rec_im = halves(flat_b, t)
            den_re.append((rec_re * own_re + rec_im * own_im).astype(jnp.bfloat16))
            den_im.append((rec_re * own_im - rec_im * own_re).astype(jnp.bfloat16))
        for b in range(FOLD):
            cells = jnp.concatenate(den_re[b : b + 2] + den_im[b : b + 2], axis=1)
            along = dot(cells, wx[b])
            for p in range(2):
                t_main[pl.ds(NG * p + DEEP * b, DEEP), :] = along[:, LANES * p : LANES * (p + 1)]
                t_edge[pl.ds(NG * p + DEEP * b, DEEP), :] = along[:, LANES * (2 + p) : LANES * (3 + p)]
        made = dot(fym[...], t_main[...].astype(jnp.bfloat16))
        side = t_edge[...]
        quads = [jnp.where(lane_quad == e, side, 0.0).astype(jnp.bfloat16) for e in range(QUADS)]
        edge = dot(fye[...], jnp.concatenate(quads, axis=0))
        for r in range(GROUPS):
            for p in range(2):
                piece = made[(2 * r + p) * FFT : (2 * r + p + 1) * FFT] if r < ROWS else edge[p * FFT : (p + 1) * FFT]
                stage[pl.ds(2 * r + p, FFT, stride=PITCH), :] = piece
        post(z, send1, recv1, a_send, a_recv)
        return carry

    lax.fori_loop(0, PLANES, forward, 0)

    everything = (slice(None), pl.ds(0, OTHERS))
    pltpu.make_async_remote_copy(
        src_ref=send1.at[everything], dst_ref=recv1.at[everything], send_sem=a_send, recv_sem=a_recv,
        device_id=(after, me), device_id_type=mesh_id,
    ).wait_recv()

    def spread(d, carry):
        for z in range(PLANES):
            acc[pl.ds(pl.multiple_of((z * FFT + d) * PITCH, 8), PIECE), :] = recv1[z, d].astype(jnp.float32)
        return carry

    lax.fori_loop(0, FFT, spread, 0)
    for r in range(GROUPS):
        runs = [acc[pl.ds(z * FFT * PITCH + 2 * r + p, FFT, stride=PITCH), :] for z in range(PLANES) for p in range(2)]
        spectrum = dot(fz[...], jnp.concatenate(runs, axis=0).astype(jnp.bfloat16))
        weight = weights[:, pl.ds(LANES * r, LANES)]
        for p in range(2):
            scaled[pl.ds(NG * p, NG), pl.ds(LANES * r, LANES)] = (spectrum[NG * p : NG * (p + 1)] * weight).astype(jnp.bfloat16)

    def give_back(z, carry):
        returned = dot(bz[pl.ds(pl.multiple_of(z * 2 * FFT, 2 * FFT), 2 * FFT), :], scaled[...])
        for r in range(GROUPS):
            for p in range(2):
                piece = returned[p * FFT : (p + 1) * FFT, LANES * r : LANES * (r + 1)]
                stage[pl.ds(2 * r + p, FFT, stride=PITCH), :] = piece
        post(z, send2, recv2, b_send, b_recv.at[z])
        return carry

    lax.fori_loop(0, PLANES, give_back, 0)

    def inverse(z, carry):
        flat_b[...] = rec[z].astype(jnp.float32)
        pltpu.make_async_remote_copy(
            src_ref=send2.at[z, pl.ds(0, OTHERS)], dst_ref=recv2.at[z, pl.ds(0, OTHERS)],
            send_sem=b_send, recv_sem=b_recv.at[z],
            device_id=(after, me), device_id_type=mesh_id,
        ).wait_recv()

        def scatter(d, inner):
            stage[pl.ds(pl.multiple_of(d * PITCH, 8), PIECE), :] = recv2[z, d].astype(jnp.float32)
            return inner

        lax.fori_loop(0, FFT, scatter, 0, unroll=8)
        runs = [stage[pl.ds(i, FFT, stride=PITCH), :] for i in range(PIECE)]
        main = jnp.concatenate(runs[: 2 * ROWS], axis=0)
        edge = jnp.concatenate(runs[2 * ROWS :], axis=0)
        quads = lane_quad[: 2 * FFT]
        edges = jnp.concatenate([jnp.where(quads == e, edge, 0.0) for e in range(QUADS)], axis=0)
        t_main[...] = dot(bym[...], main.astype(jnp.bfloat16))
        t_edge[...] = dot(bye[...], edges.astype(jnp.bfloat16))
        shares = []
        for b in range(FOLD):
            parts = [t[pl.ds(NG * p + DEEP * b, DEEP), :] for t in (t_main, t_edge) for p in range(2)]
            shares.append(dot(jnp.concatenate(parts, axis=1).astype(jnp.bfloat16), wb[b]))
        for t in range(TILES):
            field = []
            for p in range(2):
                low, high = 256 * p, 256 * p + 128
                if t == 0:
                    field.append(shares[0][:, low:high])
                elif t == FOLD:
                    field.append(shares[FOLD - 1][:, high : high + 128])
                else:
                    field.append(shares[t - 1][:, high : high + 128] + shares[t][:, low:high])
            rec_re, rec_im = halves(flat_b, t)
            flat_a[pl.ds(2 * t, DEEP, stride=2 * TILES), :] = rec_im * field[1] - rec_re * field[0]
            flat_a[pl.ds(2 * t + 1, DEEP, stride=2 * TILES), :] = -(rec_re * field[1] + rec_im * field[0])
        out[z] = flat_a[...].astype(jnp.bfloat16)
        return carry

    lax.fori_loop(0, PLANES, inverse, 0)

    for z in range(PLANES):
        shift(z).wait_send()
    for send, recv, send_sem, recv_sem in ((send1, recv1, a_send, a_recv), (send2, recv2, b_send, b_recv.at[0])):
        pltpu.make_async_remote_copy(
            src_ref=send.at[everything], dst_ref=recv.at[everything], send_sem=send_sem, recv_sem=recv_sem,
            device_id=(after, me), device_id_type=mesh_id,
        ).wait_send()


def local(orbitals, stick_map, kpoint_grid):
    orb = orbitals.reshape(2, PLANES, TILES * DEEP, LANES).transpose(1, 2, 0, 3).reshape(PLANES, RAW, LANES)
    stick = stick_map.reshape(STICK_ROWS, LANES)
    constants = tables()
    orb, stick, kgrid_t = (pltpu.with_memory_space_constraint(a, pltpu.HBM) for a in (orb, stick, kpoint_grid.T))
    constants = [pltpu.with_memory_space_constraint(c, pltpu.HBM) for c in constants]
    far = pl.BlockSpec(memory_space=pltpu.HBM)
    bf16, f32 = jnp.bfloat16, jnp.float32
    result = pl.pallas_call(
        kernel,
        name="exchange_step",
        out_shape=jax.ShapeDtypeStruct(orb.shape, bf16),
        in_specs=[far] * (3 + len(constants)),
        out_specs=pl.BlockSpec(memory_space=pltpu.VMEM),
        scratch_shapes=[
            pltpu.VMEM((3, POOL), jnp.int32),
            pltpu.VMEM(orb.shape, bf16),
            pltpu.VMEM(stick.shape, jnp.int32),
        ]
        + [pltpu.VMEM(t.shape, bf16) for t in constants]
        + [
            pltpu.VMEM((FOLD, 512, 512), bf16),
            pltpu.VMEM((FOLD, 512, 512), bf16),
            pltpu.VMEM(orb.shape, bf16),
            pltpu.VMEM((RAW, LANES), f32),
            pltpu.VMEM((RAW, LANES), f32),
            pltpu.VMEM((2 * NG, LANES), f32),
            pltpu.VMEM((2 * NG, LANES), f32),
            pltpu.VMEM((FFT * PITCH, LANES), f32),
            pltpu.VMEM((PLANES * FFT * PITCH, LANES), f32),
            pltpu.VMEM((NG, GROUPS * LANES), f32),
            pltpu.VMEM((2 * NG, GROUPS * LANES), bf16),
            pltpu.VMEM((16, 2 * LANES), f32),
        ]
        + [pltpu.VMEM((PLANES, FFT, PIECE, LANES), bf16)] * 4
        + [
            pltpu.SemaphoreType.DMA((3 + len(constants),)),
            pltpu.SemaphoreType.DMA((PLANES,)),
            pltpu.SemaphoreType.DMA((PLANES,)),
            pltpu.SemaphoreType.DMA,
            pltpu.SemaphoreType.DMA,
            pltpu.SemaphoreType.DMA,
            pltpu.SemaphoreType.DMA((PLANES,)),
        ],
        compiler_params=pltpu.CompilerParams(
            collective_id=0, has_side_effects=True, vmem_limit_bytes=48 * 1024 * 1024
        ),
    )(kgrid_t, orb, stick, *constants)
    result = result.reshape(PLANES, TILES * DEEP, 2, LANES).transpose(2, 0, 1, 3)
    return result.reshape(1, 2, 1, PLANES, NG * NG)


def solution(mesh):
    return jax.shard_map(
        local,
        mesh=mesh,
        in_specs=(P("pool", None, None, "fft", None), P(), P()),
        out_specs=P("pool", None, None, "fft", None),
        check_vma=False,
    )
```

```python
import functools
import math

import jax
import jax.numpy as jnp
import ml_dtypes
import numpy as np
from jax import lax
from jax.experimental import pallas as pl
from jax.experimental.pallas import tpu as pltpu
from jax.sharding import PartitionSpec as P

NG = 160
KMESH = 4
SPACING_BOHR = 0.1875
SCREENING = 0.106

FFT = 32
POOL = 16
PLANES = NG // FFT
ROWS = NG // FFT
QUADS = 4
FOLD = 4
DEEP = NG // FOLD
WIDE = NG * FOLD
GROUPS = ROWS + 1
PIECE = GROUPS * 2
PITCH = 72
STEPS = ((0, 3), (3, 2))
OFFSETS = (0, 40)
TILES = WIDE // 128
RAW = 2 * TILES * DEEP
OTHERS = FFT - 1
LANES = 128
STICK_ROWS = 125


def main_kx():
    lanes = np.arange(LANES)
    return np.where(lanes < 64, lanes, lanes + 32)


def edge_kx():
    return 64 + np.arange(LANES) % 32


def edge_ky():
    slots = np.arange(FFT * QUADS)
    return (slots - 64) % NG


def complex_table(inputs, outputs, orientation):
    product = (np.asarray(outputs)[:, None] * np.asarray(inputs)[None, :]) % NG
    angle = product.astype(np.float32) * np.float32(2.0 * math.pi / NG)
    cosine = np.cos(angle)
    sine = orientation * np.sin(angle)
    upper = np.stack([cosine, -sine], axis=1)
    lower = np.stack([sine, cosine], axis=1)
    return np.stack([upper, lower], axis=0).astype(np.float32)


def tables():
    folded = np.arange(NG)
    y_order = 4 * (folded % DEEP) + folded // DEEP
    grid = np.arange(NG)
    ky_main = np.arange(NG).reshape(FFT, ROWS).T.reshape(-1)
    ky_edge = edge_ky().reshape(FFT, QUADS).T.reshape(-1)
    z_order = np.arange(NG).reshape(FFT, PLANES).T.reshape(-1)

    x_main = complex_table(grid, main_kx(), -1.0)
    x_edge = complex_table(grid, edge_kx(), -1.0)
    x_all = np.stack([x_main, x_edge], axis=0)
    fx = x_all.transpose(3, 4, 0, 1, 2).reshape(2 * NG, 4 * LANES)

    def y_table(ky, n):
        full = complex_table(y_order, ky, -1.0)
        return full.reshape(2, n, FFT, 2, NG)

    fym = y_table(ky_main, ROWS).transpose(1, 0, 2, 3, 4).reshape(2 * NG, 2 * NG)
    fye = y_table(ky_edge, QUADS).transpose(0, 2, 1, 3, 4).reshape(2 * FFT, QUADS * 2 * NG)

    fz = complex_table(z_order, grid, -1.0).reshape(2, NG, 2, PLANES, FFT)
    fz = fz.transpose(0, 1, 3, 2, 4).reshape(2 * NG, 2 * NG)
    bz = complex_table(grid, z_order, 1.0).reshape(2, PLANES, FFT, 2, NG)
    bz = bz.transpose(1, 0, 2, 3, 4).reshape(2 * NG, 2 * NG)

    bym = complex_table(ky_main, y_order, 1.0).reshape(2, NG, 2, ROWS, FFT)
    bym = bym.transpose(0, 1, 3, 2, 4).reshape(2 * NG, 2 * NG)
    bye = complex_table(ky_edge, y_order, 1.0).reshape(2, NG, 2, QUADS, FFT)
    bye = bye.transpose(0, 1, 3, 2, 4).reshape(2 * NG, QUADS * 2 * FFT)

    back_main = complex_table(main_kx(), grid, 1.0)
    back_edge = complex_table(edge_kx(), grid, 1.0)
    back = np.stack([back_main, back_edge], axis=0)
    bx = back.transpose(0, 3, 4, 1, 2).reshape(4 * LANES, 2, NG)
    bx = np.pad(bx, ((0, 0), (0, 0), (0, 256 - NG))).reshape(4 * LANES, 512)
    made = (fx, fym, fye, fz, bz, bym, bye, bx)
    return [jnp.asarray(t.astype(ml_dtypes.bfloat16)) for t in made]


def signed(frequency):
    return jnp.where(frequency >= NG // 2, frequency - NG, frequency)


def dot(a, b):
    return jnp.dot(a, b, preferred_element_type=jnp.float32)


def kernel(
    kgrid_h, orb, stick_h, fx_h, fym_h, fye_h, fz_h, bz_h, bym_h, bye_h, bx_h,
    out,
    kgrid, own, stick, fx, fym, fye, fz, bz, bym, bye, bx,
    wx, wb, rec, flat_a, flat_b, t_main, t_edge, stage, weights, scaled, mask,
    send1, recv1, send2, recv2, later1, got1, later2, got2,
    load_sem, shift_send, shift_recv, a_send, a_recv, b_send, b_recv,
):
    pool = lax.axis_index("pool")
    me = lax.axis_index("fft")
    after = lax.rem(pool + 1, POOL)
    before = lax.rem(pool + POOL - 1, POOL)
    mesh_id = pl.DeviceIdType.MESH

    barrier = pltpu.get_barrier_semaphore()
    pl.semaphore_signal(barrier, inc=1, device_id=(before, me), device_id_type=mesh_id)

    def greet(k, carry):
        peer = lax.rem(me + k, FFT)
        pl.semaphore_signal(barrier, inc=1, device_id=(pool, peer), device_id_type=mesh_id)
        return carry

    lax.fori_loop(1, FFT, greet, 0)
    pairs = (
        (stick_h, stick), (kgrid_h, kgrid), (orb, own), (fx_h, fx), (bx_h, bx), (fym_h, fym),
        (fye_h, fye), (fz_h, fz), (bz_h, bz), (bym_h, bym), (bye_h, bye),
    )
    loads = [pltpu.make_async_copy(far, near, load_sem.at[i]) for i, (far, near) in enumerate(pairs)]
    for load in loads:
        load.start()
    pl.semaphore_wait(barrier, FFT)

    def shift(z):
        return pltpu.make_async_remote_copy(
            src_ref=orb.at[z], dst_ref=rec.at[z],
            send_sem=shift_send.at[z], recv_sem=shift_recv.at[z],
            device_id=(after, me), device_id_type=mesh_id,
        )

    for z in range(PLANES):
        shift(z).start()
    for load in loads:
        load.wait()

    row16 = lax.broadcasted_iota(jnp.int32, (16, LANES), 0)
    edge_row = me * QUADS + (row16 - 8) - 64
    edge_row = jnp.where(edge_row < 0, edge_row + NG, edge_row)
    own_ky = jnp.where(row16 < ROWS, me * ROWS + row16, jnp.where((row16 >= 8) & (row16 < 8 + QUADS), edge_row, -7))
    rank = lax.broadcasted_iota(jnp.int32, (2 * LANES, LANES), 0)
    kx_main = jnp.where(rank < 64, rank, rank + 32)
    kx_edge = 64 + lax.rem(rank, 32)
    every_kx = jnp.where(rank < LANES, kx_main, kx_edge)

    def count(i, total):
        hits_y, hits_x = [], []
        for u in range(5):
            slots = stick[pl.ds(5 * i + u, 1), :]
            row = slots // NG
            ky = jnp.where(slots >= 0, row, -9)
            kx = slots - row * NG
            hits_y.append(jnp.where(own_ky == ky, 1.0, 0.0))
            hits_x.append(jnp.where(every_kx == kx, 1.0, 0.0))
        hit_y = jnp.concatenate(hits_y, axis=1).astype(jnp.bfloat16)
        hit_x = jnp.concatenate(hits_x, axis=1).astype(jnp.bfloat16)
        return total + lax.dot_general(hit_y, hit_x, (((1,), (1,)), ((), ())), preferred_element_type=jnp.float32)

    mask[...] = lax.fori_loop(0, STICK_ROWS // 5, count, jnp.zeros((16, 2 * LANES), jnp.float32))

    pools = lax.broadcasted_iota(jnp.int32, (3, POOL), 1)
    moved = jnp.where(pools == pool, kgrid[...], 0) - jnp.where(pools == before, kgrid[...], 0)
    q = jnp.sum(moved.astype(jnp.float32), axis=1, keepdims=True) / KMESH
    lane = lax.broadcasted_iota(jnp.int32, (NG, LANES), 1)
    freq_z = signed(lax.broadcasted_iota(jnp.int32, (NG, LANES), 0))
    wave_z = freq_z.astype(jnp.float32) + q[2:3]
    cell = SPACING_BOHR * NG
    quad = lax.broadcasted_iota(jnp.int32, (1, LANES), 1) // 32
    for r in range(GROUPS):
        if r < ROWS:
            freq_x = jnp.where(lane < 64, lane, lane - LANES)
            freq_y = jnp.full((NG, LANES), signed(me * ROWS + r), jnp.int32)
            held = mask[pl.ds(r, 1), pl.ds(0, LANES)]
        else:
            freq_x = signed(64 + lax.rem(lane, 32))
            freq_y = me * QUADS + lane // 32 - 64
            held = jnp.zeros((1, LANES), jnp.float32)
            for e in range(QUADS):
                held = jnp.where(quad == e, mask[pl.ds(8 + e, 1), pl.ds(LANES, LANES)], held)
        inside = freq_x * freq_x + freq_y * freq_y + freq_z * freq_z <= (NG // 2) * (NG // 2)
        wave_x = freq_x.astype(jnp.float32) + q[0:1]
        wave_y = freq_y.astype(jnp.float32) + q[1:2]
        square = wave_z * wave_z + (wave_x * wave_x + wave_y * wave_y)
        exponent = math.pi * math.pi * square / (cell * cell * SCREENING * SCREENING)
        weight = cell * cell / math.pi * (1.0 - jnp.exp(-exponent)) / square / float(NG) ** 3
        weights[:, pl.ds(LANES * r, LANES)] = jnp.where(inside & (held > 0.5), weight, 0.0)

    wx[...] = jnp.zeros_like(wx)
    row_i = lax.broadcasted_iota(jnp.int32, (256, 256), 0)
    col_i = lax.broadcasted_iota(jnp.int32, (256, 256), 1)
    for b in range(FOLD):
        move = jnp.where(col_i == row_i + 32 * b, 1.0, 0.0).astype(jnp.bfloat16)
        for p in range(2):
            wx[b, pl.ds(256 * p + 32 * b, NG), :] = fx[pl.ds(NG * p, NG), :]
            wb[b, :, pl.ds(256 * p, 256)] = dot(bx[:, pl.ds(256 * p, 256)], move).astype(jnp.bfloat16)

    lane_quad = lax.broadcasted_iota(jnp.int32, (2 * NG, LANES), 1) // 32

    def row_of(z):
        return 2 * GROUPS * z + 4 * (z // 3)

    def block_to(peer, send, recv, send_sem, recv_sem):
        return pltpu.make_async_remote_copy(
            src_ref=send.at[peer], dst_ref=recv.at[me],
            send_sem=send_sem, recv_sem=recv_sem,
            device_id=(pool, peer), device_id_type=mesh_id,
        )

    def post(step, send, recv, send_sem, recv_sem):
        rows = slice(OFFSETS[step], OFFSETS[step] + PIECE * STEPS[step][1])
        send[...] = stage[...].reshape(FFT, PITCH, LANES)[:, rows].astype(jnp.bfloat16)

        def start(k, carry):
            block_to(lax.rem(me + k, FFT), send, recv, send_sem, recv_sem).start()
            return carry

        lax.fori_loop(1, FFT, start, 0)
        recv[me] = send[me]

    def others(send, recv, send_sem, recv_sem):
        part = pl.ds(0, OTHERS)
        return pltpu.make_async_remote_copy(
            src_ref=send.at[part], dst_ref=recv.at[part], send_sem=send_sem, recv_sem=recv_sem,
            device_id=(after, me), device_id_type=mesh_id,
        )

    def collect(step, send, recv, send_sem, recv_sem):
        others(send, recv, send_sem, recv_sem).wait_recv()

        def spread(d, carry):
            start = pl.multiple_of(d * PITCH + OFFSETS[step], 8)
            stage[pl.ds(start, PIECE * STEPS[step][1]), :] = recv[d].astype(jnp.float32)
            return carry

        lax.fori_loop(0, FFT, spread, 0, unroll=4)

    out_legs = ((send1, recv1, a_send.at[0], a_recv.at[0]), (later1, got1, a_send.at[1], a_recv.at[1]))
    back_legs = ((send2, recv2, b_send.at[0], b_recv.at[0]), (later2, got2, b_send.at[1], b_recv.at[1]))

    def halves(source, t):
        return [source[pl.ds(2 * t + p, DEEP, stride=2 * TILES), :] for p in range(2)]

    def forward(z, carry):
        flat_a[...] = own[z].astype(jnp.float32)
        shift(z).wait_recv()
        flat_b[...] = rec[z].astype(jnp.float32)
        den_re, den_im = [], []
        for t in range(TILES):
            own_re, own_im = halves(flat_a, t)
            rec_re, rec_im = halves(flat_b, t)
            den_re.append((rec_re * own_re + rec_im * own_im).astype(jnp.bfloat16))
            den_im.append((rec_re * own_im - rec_im * own_re).astype(jnp.bfloat16))
        for b in range(FOLD):
            cells = jnp.concatenate(den_re[b : b + 2] + den_im[b : b + 2], axis=1)
            along = dot(cells, wx[b])
            for p in range(2):
                t_main[pl.ds(NG * p + DEEP * b, DEEP), :] = along[:, LANES * p : LANES * (p + 1)]
                t_edge[pl.ds(NG * p + DEEP * b, DEEP), :] = along[:, LANES * (2 + p) : LANES * (3 + p)]
        made = dot(fym[...], t_main[...].astype(jnp.bfloat16))
        side = t_edge[...]
        quads = [jnp.where(lane_quad == e, side, 0.0).astype(jnp.bfloat16) for e in range(QUADS)]
        edge = dot(fye[...], jnp.concatenate(quads, axis=0))
        for r in range(GROUPS):
            for p in range(2):
                piece = made[(2 * r + p) * FFT : (2 * r + p + 1) * FFT] if r < ROWS else edge[p * FFT : (p + 1) * FFT]
                stage[pl.ds(row_of(z) + 2 * r + p, FFT, stride=PITCH), :] = piece
        return carry

    for step, (first, count_z) in enumerate(STEPS):
        lax.fori_loop(first, first + count_z, forward, 0)
        post(step, *out_legs[step])

    for step in range(2):
        collect(step, *out_legs[step])
    for r in range(GROUPS):
        runs = [stage[pl.ds(row_of(z) + 2 * r + p, FFT, stride=PITCH), :] for z in range(PLANES) for p in range(2)]
        spectrum = dot(fz[...], jnp.concatenate(runs, axis=0).astype(jnp.bfloat16))
        weight = weights[:, pl.ds(LANES * r, LANES)]
        for p in range(2):
            scaled[pl.ds(NG * p, NG), pl.ds(LANES * r, LANES)] = (spectrum[NG * p : NG * (p + 1)] * weight).astype(jnp.bfloat16)

    def give_back(z, carry):
        returned = dot(bz[pl.ds(pl.multiple_of(z * 2 * FFT, 2 * FFT), 2 * FFT), :], scaled[...])
        for r in range(GROUPS):
            for p in range(2):
                piece = returned[p * FFT : (p + 1) * FFT, LANES * r : LANES * (r + 1)]
                stage[pl.ds(row_of(z) + 2 * r + p, FFT, stride=PITCH), :] = piece
        return carry

    for step, (first, count_z) in enumerate(STEPS):
        lax.fori_loop(first, first + count_z, give_back, 0)
        post(step, *back_legs[step])

    def inverse(z, carry):
        flat_b[...] = rec[z].astype(jnp.float32)
        base = row_of(z)
        runs = [stage[pl.ds(base + i, FFT, stride=PITCH), :] for i in range(PIECE)]
        main = jnp.concatenate(runs[: 2 * ROWS], axis=0)
        edge = jnp.concatenate(runs[2 * ROWS :], axis=0)
        quads = lane_quad[: 2 * FFT]
        edges = jnp.concatenate([jnp.where(quads == e, edge, 0.0) for e in range(QUADS)], axis=0)
        t_main[...] = dot(bym[...], main.astype(jnp.bfloat16))
        t_edge[...] = dot(bye[...], edges.astype(jnp.bfloat16))
        shares = []
        for b in range(FOLD):
            parts = [t[pl.ds(NG * p + DEEP * b, DEEP), :] for t in (t_main, t_edge) for p in range(2)]
            shares.append(dot(jnp.concatenate(parts, axis=1).astype(jnp.bfloat16), wb[b]))
        for t in range(TILES):
            field = []
            for p in range(2):
                low, high = 256 * p, 256 * p + 128
                if t == 0:
                    field.append(shares[0][:, low:high])
                elif t == FOLD:
                    field.append(shares[FOLD - 1][:, high : high + 128])
                else:
                    field.append(shares[t - 1][:, high : high + 128] + shares[t][:, low:high])
            rec_re, rec_im = halves(flat_b, t)
            flat_a[pl.ds(2 * t, DEEP, stride=2 * TILES), :] = rec_im * field[1] - rec_re * field[0]
            flat_a[pl.ds(2 * t + 1, DEEP, stride=2 * TILES), :] = -(rec_re * field[1] + rec_im * field[0])
        out[z] = flat_a[...].astype(jnp.bfloat16)
        return carry

    for step, (first, count_z) in enumerate(STEPS):
        collect(step, *back_legs[step])
        lax.fori_loop(first, first + count_z, inverse, 0)

    for z in range(PLANES):
        shift(z).wait_send()
    for leg in out_legs + back_legs:
        others(*leg).wait_send()


def local(orbitals, stick_map, kpoint_grid):
    orb = orbitals.reshape(2, PLANES, TILES * DEEP, LANES).transpose(1, 2, 0, 3).reshape(PLANES, RAW, LANES)
    stick = stick_map.reshape(STICK_ROWS, LANES)
    constants = tables()
    orb, stick, kgrid_t = (pltpu.with_memory_space_constraint(a, pltpu.HBM) for a in (orb, stick, kpoint_grid.T))
    constants = [pltpu.with_memory_space_constraint(c, pltpu.HBM) for c in constants]
    far = pl.BlockSpec(memory_space=pltpu.HBM)
    bf16, f32 = jnp.bfloat16, jnp.float32
    result = pl.pallas_call(
        kernel,
        name="exchange_step",
        out_shape=jax.ShapeDtypeStruct(orb.shape, bf16),
        in_specs=[far] * (3 + len(constants)),
        out_specs=pl.BlockSpec(memory_space=pltpu.VMEM),
        scratch_shapes=[
            pltpu.VMEM((3, POOL), jnp.int32),
            pltpu.VMEM(orb.shape, bf16),
            pltpu.VMEM(stick.shape, jnp.int32),
        ]
        + [pltpu.VMEM(t.shape, bf16) for t in constants]
        + [
            pltpu.VMEM((FOLD, 512, 512), bf16),
            pltpu.VMEM((FOLD, 512, 512), bf16),
            pltpu.VMEM(orb.shape, bf16),
            pltpu.VMEM((RAW, LANES), f32),
            pltpu.VMEM((RAW, LANES), f32),
            pltpu.VMEM((2 * NG, LANES), f32),
            pltpu.VMEM((2 * NG, LANES), f32),
            pltpu.VMEM((FFT * PITCH, LANES), f32),
            pltpu.VMEM((NG, GROUPS * LANES), f32),
            pltpu.VMEM((2 * NG, GROUPS * LANES), bf16),
            pltpu.VMEM((16, 2 * LANES), f32),
        ]
        + [pltpu.VMEM((FFT, PIECE * n, LANES), bf16) for _, n in STEPS for _ in range(4)]
        + [
            pltpu.SemaphoreType.DMA((3 + len(constants),)),
            pltpu.SemaphoreType.DMA((PLANES,)),
            pltpu.SemaphoreType.DMA((PLANES,)),
        ]
        + [pltpu.SemaphoreType.DMA((2,))] * 4,
        compiler_params=pltpu.CompilerParams(
            collective_id=0, has_side_effects=True, vmem_limit_bytes=48 * 1024 * 1024
        ),
    )(kgrid_t, orb, stick, *constants)
    result = result.reshape(PLANES, TILES * DEEP, 2, LANES).transpose(2, 0, 1, 3)
    return result.reshape(1, 2, 1, PLANES, NG * NG)


def solution(mesh):
    return jax.shard_map(
        local,
        mesh=mesh,
        in_specs=(P("pool", None, None, "fft", None), P(), P()),
        out_specs=P("pool", None, None, "fft", None),
        check_vma=False,
    )
```

```python
import functools
import math

import jax
import jax.numpy as jnp
import ml_dtypes
import numpy as np
from jax import lax
from jax.experimental import pallas as pl
from jax.experimental.pallas import tpu as pltpu
from jax.sharding import PartitionSpec as P

NG = 160
KMESH = 4
SPACING_BOHR = 0.1875
SCREENING = 0.106

FFT = 32
POOL = 16
PLANES = NG // FFT
ROWS = NG // FFT
QUADS = 4
EDGE_SHIFT = (-48, -16, 31, 15)
FOLD = 4
DEEP = NG // FOLD
WIDE = NG * FOLD
GROUPS = ROWS + 1
PITCH = 72
OUT_ROWS = ((0, 32), (32, 24))
BACK_ROWS = ((0, 40), (40, 16))
SHARE = 2 * ROWS + 1
HALF = 64
LATE = 14
TILES = WIDE // 128
RAW = 2 * TILES * DEEP
OTHERS = FFT - 1
LANES = 128
STICK_ROWS = 125


def kx_of(quad, place):
    return np.where(place < 16, 16 * quad + place, place - 32 - 16 * quad)


def main_kx():
    lanes = np.arange(LANES)
    return kx_of(lanes // 32, lanes % 32)


def edge_kx():
    return kx_of(QUADS, np.arange(LANES) % 32)


def main_ky():
    near = np.arange((ROWS - 1) * FFT).reshape(FFT, ROWS - 1).T
    near = np.where(near < 64, near, near + 32)
    return np.concatenate([near, 64 + np.arange(FFT)[None]], axis=0).reshape(-1)


def edge_ky():
    return (np.array(EDGE_SHIFT)[:, None] + np.arange(FFT)[None]).reshape(-1)


def complex_table(inputs, outputs, orientation):
    product = (np.asarray(outputs)[:, None] * np.asarray(inputs)[None, :]) % NG
    angle = product.astype(np.float32) * np.float32(2.0 * math.pi / NG)
    cosine = np.cos(angle)
    sine = orientation * np.sin(angle)
    upper = np.stack([cosine, -sine], axis=1)
    lower = np.stack([sine, cosine], axis=1)
    return np.stack([upper, lower], axis=0).astype(np.float32)


def tables():
    folded = np.arange(NG)
    y_order = 4 * (folded % DEEP) + folded // DEEP
    grid = np.arange(NG)
    ky_main = main_ky()
    ky_edge = edge_ky()
    z_order = np.arange(NG).reshape(FFT, PLANES).T.reshape(-1)

    x_main = complex_table(grid, main_kx(), -1.0)
    x_edge = complex_table(grid, edge_kx(), -1.0)
    x_all = np.stack([x_main, x_edge], axis=0)
    fx = x_all.transpose(3, 4, 0, 1, 2).reshape(2 * NG, 4 * LANES)

    def y_table(ky, n):
        full = complex_table(y_order, ky, -1.0)
        return full.reshape(2, n, FFT, 2, NG)

    fym = y_table(ky_main, ROWS).transpose(1, 0, 2, 3, 4).reshape(2 * NG, 2 * NG)
    fye = y_table(ky_edge, QUADS).transpose(0, 2, 1, 3, 4).reshape(2 * FFT, QUADS * 2 * NG)

    fz = complex_table(z_order, grid, -1.0).reshape(2, NG, 2, PLANES, FFT)
    fz = fz.transpose(0, 1, 3, 2, 4).reshape(2 * NG, 2 * NG)
    bz = complex_table(grid, z_order, 1.0).reshape(2, PLANES, FFT, 2, NG)
    bz = bz.transpose(1, 0, 2, 3, 4).reshape(2 * NG, 2 * NG)

    bym = complex_table(ky_main, y_order, 1.0).reshape(2, NG, 2, ROWS, FFT)
    bym = bym.transpose(0, 1, 3, 2, 4).reshape(2 * NG, 2 * NG)
    bye = complex_table(ky_edge, y_order, 1.0).reshape(2, NG, 2, QUADS, FFT)
    bye = bye.transpose(0, 1, 3, 2, 4).reshape(2 * NG, QUADS * 2 * FFT)

    back_main = complex_table(main_kx(), grid, 1.0)
    back_edge = complex_table(edge_kx(), grid, 1.0)
    back = np.stack([back_main, back_edge], axis=0)
    bx = back.transpose(0, 3, 4, 1, 2).reshape(4 * LANES, 2, NG)
    bx = np.pad(bx, ((0, 0), (0, 0), (0, 256 - NG))).reshape(4 * LANES, 512)
    made = (fx, fym, fye, fz, bz, bym, bye, bx)
    return [jnp.asarray(t.astype(ml_dtypes.bfloat16)) for t in made]


def signed(frequency):
    return jnp.where(frequency >= NG // 2, frequency - NG, frequency)


def signed_kx(quad, place):
    return jnp.where(place < 16, 16 * quad + place, place - 32 - 16 * quad)


def edge_shift(quad):
    shift = jnp.where(quad == 0, EDGE_SHIFT[0], EDGE_SHIFT[1])
    return jnp.where(quad == 2, EDGE_SHIFT[2], jnp.where(quad == 3, EDGE_SHIFT[3], shift))


def lent(device, quad):
    return ((quad == 3) & (device >= 1)) | ((quad == 2) & ((device == 16) | (device == 17)))


def dot(a, b):
    return jnp.dot(a, b, preferred_element_type=jnp.float32)


def kernel(
    kgrid_h, orb, stick_h, fx_h, fym_h, fye_h, fz_h, bz_h, bym_h, bye_h, bx_h,
    out,
    kgrid, own, stick, fx, fym, fye, fz, bz, bym, bye, bx,
    wx, rec, flat_a, flat_b, stage, weights, mask,
    send1, recv1, send2, recv2, later1, got1, later2, got2,
    load_sem, shift_send, shift_recv, a_send, a_recv, b_send, b_recv,
):
    pool = lax.axis_index("pool")
    me = lax.axis_index("fft")
    after = lax.rem(pool + 1, POOL)
    before = lax.rem(pool + POOL - 1, POOL)
    mesh_id = pl.DeviceIdType.MESH

    barrier = pltpu.get_barrier_semaphore()
    pl.semaphore_signal(barrier, inc=1, device_id=(before, me), device_id_type=mesh_id)

    def greet(k, carry):
        peer = lax.rem(me + k, FFT)
        pl.semaphore_signal(barrier, inc=1, device_id=(pool, peer), device_id_type=mesh_id)
        return carry

    lax.fori_loop(1, FFT, greet, 0)
    pairs = (
        (stick_h, stick), (kgrid_h, kgrid), (orb, own), (fx_h, fx), (bx_h, bx), (fym_h, fym),
        (fye_h, fye), (fz_h, fz), (bz_h, bz), (bym_h, bym), (bye_h, bye),
    )
    loads = [pltpu.make_async_copy(far, near, load_sem.at[i]) for i, (far, near) in enumerate(pairs)]
    for load in loads:
        load.start()
    pl.semaphore_wait(barrier, FFT)

    def shift(z):
        return pltpu.make_async_remote_copy(
            src_ref=orb.at[z], dst_ref=rec.at[z],
            send_sem=shift_send.at[z], recv_sem=shift_recv.at[z],
            device_id=(after, me), device_id_type=mesh_id,
        )

    for z in range(PLANES):
        shift(z).start()
    for load in loads:
        load.wait()

    row16 = lax.broadcasted_iota(jnp.int32, (16, LANES), 0)
    near_row = me * (ROWS - 1) + row16
    near_row = jnp.where(near_row < 64, near_row, near_row + 32)
    near_row = jnp.where(row16 < ROWS - 1, near_row, 64 + me)
    edge_row = me + edge_shift(row16 - 8)
    edge_row = jnp.where(edge_row < 0, edge_row + NG, edge_row)
    own_ky = jnp.where(row16 < ROWS, near_row, jnp.where((row16 >= 8) & (row16 < 8 + QUADS), edge_row, -7))
    rank = lax.broadcasted_iota(jnp.int32, (2 * LANES, LANES), 0)
    every_kx = signed_kx(jnp.where(rank < LANES, rank // 32, QUADS), lax.rem(rank, 32))
    every_kx = jnp.where(every_kx < 0, every_kx + NG, every_kx)

    def count(i, total):
        hits_y, hits_x = [], []
        for u in range(5):
            slots = stick[pl.ds(5 * i + u, 1), :]
            row = slots // NG
            ky = jnp.where(slots >= 0, row, -9)
            kx = slots - row * NG
            hits_y.append(jnp.where(own_ky == ky, 1.0, 0.0))
            hits_x.append(jnp.where(every_kx == kx, 1.0, 0.0))
        hit_y = jnp.concatenate(hits_y, axis=1).astype(jnp.bfloat16)
        hit_x = jnp.concatenate(hits_x, axis=1).astype(jnp.bfloat16)
        return total + lax.dot_general(hit_y, hit_x, (((1,), (1,)), ((), ())), preferred_element_type=jnp.float32)

    mask[...] = lax.fori_loop(0, STICK_ROWS // 5, count, jnp.zeros((16, 2 * LANES), jnp.float32))

    pools = lax.broadcasted_iota(jnp.int32, (3, POOL), 1)
    moved = jnp.where(pools == pool, kgrid[...], 0) - jnp.where(pools == before, kgrid[...], 0)
    q = jnp.sum(moved.astype(jnp.float32), axis=1, keepdims=True) / KMESH
    lane = lax.broadcasted_iota(jnp.int32, (NG, LANES), 1)
    freq_z = signed(lax.broadcasted_iota(jnp.int32, (NG, LANES), 0))
    wave_z = freq_z.astype(jnp.float32) + q[2:3]
    cell = SPACING_BOHR * NG
    quad = lax.broadcasted_iota(jnp.int32, (1, LANES), 1) // 32
    outer_held = jnp.zeros((1, LANES), jnp.float32)
    for e in range(QUADS):
        outer_held = jnp.where(quad == e, mask[pl.ds(8 + e, 1), pl.ds(LANES, LANES)], outer_held)
    outer_x = signed_kx(QUADS, lax.rem(lane, 32))
    outer_y = me + edge_shift(lane // 32)
    for r in range(GROUPS):
        if r < ROWS - 1:
            near = me * (ROWS - 1) + r
            freq_x = signed_kx(lane // 32, lax.rem(lane, 32))
            freq_y = jnp.full((NG, LANES), signed(jnp.where(near < 64, near, near + 32)), jnp.int32)
            held = mask[pl.ds(r, 1), pl.ds(0, LANES)]
        elif r < ROWS:
            freq_x = jnp.where(lent(me, lane // 32), outer_x, signed_kx(lane // 32, lax.rem(lane, 32)))
            freq_y = jnp.where(lent(me, lane // 32), outer_y, signed(64 + me))
            held = jnp.where(lent(me, quad), outer_held, mask[pl.ds(r, 1), pl.ds(0, LANES)])
        else:
            freq_x, freq_y = outer_x, outer_y
            held = jnp.where(quad < 2, outer_held, 0.0)
        inside = freq_x * freq_x + freq_y * freq_y + freq_z * freq_z <= (NG // 2) * (NG // 2)
        wave_x = freq_x.astype(jnp.float32) + q[0:1]
        wave_y = freq_y.astype(jnp.float32) + q[1:2]
        square = wave_z * wave_z + (wave_x * wave_x + wave_y * wave_y)
        exponent = math.pi * math.pi * square / (cell * cell * SCREENING * SCREENING)
        weight = cell * cell / math.pi * (1.0 - jnp.exp(-exponent)) / square / float(NG) ** 3
        weights[:, pl.ds(LANES * r, LANES)] = jnp.where(inside & (held > 0.5), weight, 0.0)

    wx[...] = jnp.zeros_like(wx)
    for p in range(2):
        wx[pl.ds(256 * p, NG), :] = fx[pl.ds(NG * p, NG), :]

    lane_quad = lax.broadcasted_iota(jnp.int32, (2 * NG, LANES), 1) // 32

    small_lane = lax.broadcasted_iota(jnp.int32, (FFT, LANES), 1)
    small_lent = lent(lax.broadcasted_iota(jnp.int32, (FFT, LANES), 0), small_lane // 32)

    def joined(real, imaginary):
        return jnp.where(small_lane < HALF, real, pltpu.roll(imaginary, HALF, axis=1))

    def block_to(peer, send, recv, send_sem, recv_sem):
        return pltpu.make_async_remote_copy(
            src_ref=send.at[peer], dst_ref=recv.at[me],
            send_sem=send_sem, recv_sem=recv_sem,
            device_id=(pool, peer), device_id_type=mesh_id,
        )

    def post(rows, send, recv, send_sem, recv_sem):
        rows = slice(rows[0], rows[0] + rows[1])
        send[...] = stage[...].reshape(FFT, PITCH, LANES)[:, rows].astype(jnp.bfloat16)

        def start(k, carry):
            block_to(lax.rem(me + k, FFT), send, recv, send_sem, recv_sem).start()
            return carry

        lax.fori_loop(1, FFT, start, 0)
        recv[me] = send[me]

    def others(send, recv, send_sem, recv_sem):
        part = pl.ds(0, OTHERS)
        return pltpu.make_async_remote_copy(
            src_ref=send.at[part], dst_ref=recv.at[part], send_sem=send_sem, recv_sem=recv_sem,
            device_id=(after, me), device_id_type=mesh_id,
        )

    def collect(rows, send, recv, send_sem, recv_sem):
        others(send, recv, send_sem, recv_sem).wait_recv()

        def spread(d, carry):
            start = pl.multiple_of(d * PITCH + rows[0], 8)
            stage[pl.ds(start, rows[1]), :] = recv[d].astype(jnp.float32)
            return carry

        lax.fori_loop(0, FFT, spread, 0, unroll=4)

    out_legs = ((send1, recv1, a_send.at[0], a_recv.at[0]), (later1, got1, a_send.at[1], a_recv.at[1]))
    back_legs = ((send2, recv2, b_send.at[0], b_recv.at[0]), (later2, got2, b_send.at[1], b_recv.at[1]))

    def halves(source, t):
        return [source[pl.ds(2 * t + p, DEEP, stride=2 * TILES), :] for p in range(2)]

    def forward(z, carry):
        flat_a[...] = own[z].astype(jnp.float32)
        shift(z).wait_recv()
        flat_b[...] = rec[z].astype(jnp.float32)
        den_re, den_im = [], []
        for t in range(TILES):
            own_re, own_im = halves(flat_a, t)
            rec_re, rec_im = halves(flat_b, t)
            den_re.append(rec_re * own_re + rec_im * own_im)
            den_im.append(rec_re * own_im - rec_im * own_re)
        runs = []
        for b in range(FOLD):
            parts = [jnp.concatenate(den[b : b + 2], axis=1) for den in (den_re, den_im)]
            if b > 0:
                parts = [pltpu.roll(part, 256 - 32 * b, axis=1) for part in parts]
            runs.append(jnp.concatenate(parts, axis=1))
        along = dot(jnp.concatenate(runs, axis=0).astype(jnp.bfloat16), wx[...])
        planes = [along[:, LANES * k : LANES * (k + 1)] for k in range(4)]
        made = dot(fym[...], jnp.concatenate(planes[:2], axis=0).astype(jnp.bfloat16))
        side = jnp.concatenate(planes[2:], axis=0)
        quads = [jnp.where(lane_quad == e, side, 0.0).astype(jnp.bfloat16) for e in range(QUADS)]
        edge = dot(fye[...], jnp.concatenate(quads, axis=0))
        edges = [edge[p * FFT : (p + 1) * FFT] for p in range(2)]
        for r in range(ROWS):
            for p in range(2):
                piece = made[(2 * r + p) * FFT : (2 * r + p + 1) * FFT]
                if r == ROWS - 1:
                    piece = jnp.where(small_lent, edges[p], piece)
                stage[pl.ds(SHARE * z + 2 * r + p, FFT, stride=PITCH), :] = piece
        stage[pl.ds(SHARE * z + 2 * ROWS, FFT, stride=PITCH), :] = joined(*edges)
        return carry

    lax.fori_loop(0, 3, forward, 0)

    @pl.when(pool < LATE)
    def _():
        post(OUT_ROWS[0], *out_legs[0])

    lax.fori_loop(3, PLANES, forward, 0)

    @pl.when(pool >= LATE)
    def _():
        post(OUT_ROWS[0], *out_legs[0])

    post(OUT_ROWS[1], *out_legs[1])

    for step in range(2):
        collect(OUT_ROWS[step], *out_legs[step])
    for first in range(0, GROUPS, 2):
        fields = []
        for r in (first, first + 1):
            if r < ROWS:
                runs = [stage[pl.ds(SHARE * z + 2 * r + p, FFT, stride=PITCH), :] for z in range(PLANES) for p in range(2)]
            else:
                both = [stage[pl.ds(SHARE * z + 2 * ROWS, FFT, stride=PITCH), :] for z in range(PLANES)]
                runs = [part for row in both for part in (row, pltpu.roll(row, HALF, axis=1))]
            fields.append(jnp.concatenate(runs, axis=0))
        spectrum = dot(fz[...], jnp.concatenate(fields, axis=1).astype(jnp.bfloat16))
        weight = weights[:, pl.ds(LANES * first, 2 * LANES)]
        scaled = jnp.concatenate([spectrum[:NG] * weight, spectrum[NG:] * weight], axis=0).astype(jnp.bfloat16)
        returned = dot(bz[...], scaled)
        for r in (first, first + 1):
            part = returned[:, LANES * (r - first) : LANES * (r - first + 1)]
            for z in range(PLANES):
                pair = [part[FFT * (2 * z + p) : FFT * (2 * z + p + 1)] for p in range(2)]
                if r < ROWS:
                    for p in range(2):
                        stage[pl.ds(SHARE * z + 2 * r + p, FFT, stride=PITCH), :] = pair[p]
                else:
                    stage[pl.ds(SHARE * z + 2 * ROWS, FFT, stride=PITCH), :] = joined(*pair)

    post(BACK_ROWS[0], *back_legs[0])
    post(BACK_ROWS[1], *back_legs[1])

    def inverse(z, carry):
        flat_b[...] = rec[z].astype(jnp.float32)
        runs = [stage[pl.ds(SHARE * z + i, FFT, stride=PITCH), :] for i in range(SHARE)]
        half_row = (runs[2 * ROWS], pltpu.roll(runs[2 * ROWS], HALF, axis=1))
        last = runs[2 * ROWS - 2 : 2 * ROWS]
        kept = [jnp.where(small_lent, 0.0, row) for row in last]
        main = jnp.concatenate(runs[: 2 * ROWS - 2] + kept, axis=0)
        edge = [jnp.where(small_lane < HALF, half_row[p], jnp.where(small_lent, last[p], 0.0)) for p in range(2)]
        edge = jnp.concatenate(edge, axis=0)
        quads = lane_quad[: 2 * FFT]
        edges = jnp.concatenate([jnp.where(quads == e, edge, 0.0) for e in range(QUADS)], axis=0)
        columns = [dot(bym[...], main.astype(jnp.bfloat16)), dot(bye[...], edges.astype(jnp.bfloat16))]
        parts = [column[NG * p : NG * (p + 1)] for column in columns for p in range(2)]
        along = dot(jnp.concatenate(parts, axis=1).astype(jnp.bfloat16), bx[...])
        shares = []
        for b in range(FOLD):
            windows = [along[DEEP * b : DEEP * (b + 1), 256 * p : 256 * (p + 1)] for p in range(2)]
            if b > 0:
                windows = [pltpu.roll(window, 32 * b, axis=1) for window in windows]
            shares.append(jnp.concatenate(windows, axis=1))
        for t in range(TILES):
            field = []
            for p in range(2):
                low, high = 256 * p, 256 * p + 128
                if t == 0:
                    field.append(shares[0][:, low:high])
                elif t == FOLD:
                    field.append(shares[FOLD - 1][:, high : high + 128])
                else:
                    field.append(shares[t - 1][:, high : high + 128] + shares[t][:, low:high])
            rec_re, rec_im = halves(flat_b, t)
            flat_a[pl.ds(2 * t, DEEP, stride=2 * TILES), :] = rec_im * field[1] - rec_re * field[0]
            flat_a[pl.ds(2 * t + 1, DEEP, stride=2 * TILES), :] = -(rec_re * field[1] + rec_im * field[0])
        out[z] = flat_a[...].astype(jnp.bfloat16)
        return carry

    collect(BACK_ROWS[0], *back_legs[0])
    lax.fori_loop(0, 3, inverse, 0)
    collect(BACK_ROWS[1], *back_legs[1])
    lax.fori_loop(3, PLANES, inverse, 0)

    for z in range(PLANES):
        shift(z).wait_send()
    for leg in out_legs + back_legs:
        others(*leg).wait_send()


def local(orbitals, stick_map, kpoint_grid):
    orb = orbitals.reshape(2, PLANES, TILES * DEEP, LANES).transpose(1, 2, 0, 3).reshape(PLANES, RAW, LANES)
    stick = stick_map.reshape(STICK_ROWS, LANES)
    constants = tables()
    orb, stick, kgrid_t = (pltpu.with_memory_space_constraint(a, pltpu.HBM) for a in (orb, stick, kpoint_grid.T))
    constants = [pltpu.with_memory_space_constraint(c, pltpu.HBM) for c in constants]
    far = pl.BlockSpec(memory_space=pltpu.HBM)
    bf16, f32 = jnp.bfloat16, jnp.float32
    result = pl.pallas_call(
        kernel,
        name="exchange_step",
        out_shape=jax.ShapeDtypeStruct(orb.shape, bf16),
        in_specs=[far] * (3 + len(constants)),
        out_specs=pl.BlockSpec(memory_space=pltpu.VMEM),
        scratch_shapes=[
            pltpu.VMEM((3, POOL), jnp.int32),
            pltpu.VMEM(orb.shape, bf16),
            pltpu.VMEM(stick.shape, jnp.int32),
        ]
        + [pltpu.VMEM(t.shape, bf16) for t in constants]
        + [
            pltpu.VMEM((512, 512), bf16),
            pltpu.VMEM(orb.shape, bf16),
            pltpu.VMEM((RAW, LANES), f32),
            pltpu.VMEM((RAW, LANES), f32),
            pltpu.VMEM((FFT * PITCH, LANES), f32),
            pltpu.VMEM((NG, GROUPS * LANES), f32),
            pltpu.VMEM((16, 2 * LANES), f32),
        ]
        + [pltpu.VMEM((FFT, rows[k][1], LANES), bf16) for k in range(2) for rows in (OUT_ROWS, OUT_ROWS, BACK_ROWS, BACK_ROWS)]
        + [
            pltpu.SemaphoreType.DMA((3 + len(constants),)),
            pltpu.SemaphoreType.DMA((PLANES,)),
            pltpu.SemaphoreType.DMA((PLANES,)),
        ]
        + [pltpu.SemaphoreType.DMA((2,))] * 4,
        compiler_params=pltpu.CompilerParams(
            collective_id=0, has_side_effects=True, vmem_limit_bytes=48 * 1024 * 1024
        ),
    )(kgrid_t, orb, stick, *constants)
    result = result.reshape(PLANES, TILES * DEEP, 2, LANES).transpose(2, 0, 1, 3)
    return result.reshape(1, 2, 1, PLANES, NG * NG)


def solution(mesh):
    return jax.shard_map(
        local,
        mesh=mesh,
        in_specs=(P("pool", None, None, "fft", None), P(), P()),
        out_specs=P("pool", None, None, "fft", None),
        check_vma=False,
    )
```

```python
import functools
import math

import jax
import jax.numpy as jnp
import ml_dtypes
import numpy as np
from jax import lax
from jax.experimental import pallas as pl
from jax.experimental.pallas import tpu as pltpu
from jax.sharding import PartitionSpec as P

NG = 160
KMESH = 4
SPACING_BOHR = 0.1875
SCREENING = 0.106

FFT = 32
POOL = 16
PLANES = NG // FFT
ROWS = NG // FFT
QUADS = 4
EDGE_SHIFT = (-48, -16, 31, 15)
FOLD = 4
DEEP = NG // FOLD
WIDE = NG * FOLD
GROUPS = ROWS + 1
PITCH = 72
OUT_ROWS = ((0, 32), (32, 24))
BACK_ROWS = ((0, 40), (40, 16))
SHARE = 2 * ROWS + 1
HALF = 64
LATE = 14
TILES = WIDE // 128
RAW = 2 * TILES * DEEP
OTHERS = FFT - 1
LANES = 128
STICK_ROWS = 125


def kx_of(quad, place):
    return np.where(place < 16, 16 * quad + place, place - 32 - 16 * quad)


def main_kx():
    lanes = np.arange(LANES)
    return kx_of(lanes // 32, lanes % 32)


def edge_kx():
    return kx_of(QUADS, np.arange(LANES) % 32)


def main_ky():
    near = np.arange((ROWS - 1) * FFT).reshape(FFT, ROWS - 1).T
    near = np.where(near < 64, near, near + 32)
    return np.concatenate([near, 64 + np.arange(FFT)[None]], axis=0).reshape(-1)


def edge_ky():
    return (np.array(EDGE_SHIFT)[:, None] + np.arange(FFT)[None]).reshape(-1)


def complex_table(inputs, outputs, orientation):
    product = (np.asarray(outputs)[:, None] * np.asarray(inputs)[None, :]) % NG
    angle = product.astype(np.float32) * np.float32(2.0 * math.pi / NG)
    cosine = np.cos(angle)
    sine = orientation * np.sin(angle)
    upper = np.stack([cosine, -sine], axis=1)
    lower = np.stack([sine, cosine], axis=1)
    return np.stack([upper, lower], axis=0).astype(np.float32)


def tables():
    folded = np.arange(NG)
    y_order = 4 * (folded % DEEP) + folded // DEEP
    grid = np.arange(NG)
    ky_main = main_ky()
    ky_edge = edge_ky()
    z_order = np.arange(NG).reshape(FFT, PLANES).T.reshape(-1)

    x_main = complex_table(grid, main_kx(), -1.0)
    x_edge = complex_table(grid, edge_kx(), -1.0)
    x_all = np.stack([x_main, x_edge], axis=0)
    fx = x_all.transpose(3, 4, 0, 1, 2).reshape(2 * NG, 4 * LANES)

    def y_table(ky, n):
        full = complex_table(y_order, ky, -1.0)
        return full.reshape(2, n, FFT, 2, NG)

    fym = y_table(ky_main, ROWS).transpose(1, 0, 2, 3, 4).reshape(2 * NG, 2 * NG)
    fye = y_table(ky_edge, QUADS).transpose(0, 2, 1, 3, 4).reshape(2 * FFT, QUADS * 2 * NG)

    fz = complex_table(z_order, grid, -1.0).reshape(2, NG, 2, PLANES, FFT)
    fz = fz.transpose(0, 1, 3, 2, 4).reshape(2 * NG, 2 * NG)
    bz = complex_table(grid, z_order, 1.0).reshape(2, PLANES, FFT, 2, NG)
    bz = bz.transpose(1, 0, 2, 3, 4).reshape(2 * NG, 2 * NG)

    bym = complex_table(ky_main, y_order, 1.0).reshape(2, NG, 2, ROWS, FFT)
    bym = bym.transpose(0, 1, 3, 2, 4).reshape(2 * NG, 2 * NG)
    bye = complex_table(ky_edge, y_order, 1.0).reshape(2, NG, 2, QUADS, FFT)
    bye = bye.transpose(0, 1, 3, 2, 4).reshape(2 * NG, QUADS * 2 * FFT)

    back_main = complex_table(main_kx(), grid, 1.0)
    back_edge = complex_table(edge_kx(), grid, 1.0)
    back = np.stack([back_main, back_edge], axis=0)
    bx = back.transpose(0, 3, 4, 1, 2).reshape(4 * LANES, 2, NG)
    bx = np.pad(bx, ((0, 0), (0, 0), (0, 256 - NG))).reshape(4 * LANES, 512)
    made = (fx, fym, fye, fz, bz, bym, bye, bx)
    return [jnp.asarray(t.astype(ml_dtypes.bfloat16)) for t in made]


def signed(frequency):
    return jnp.where(frequency >= NG // 2, frequency - NG, frequency)


def signed_kx(quad, place):
    return jnp.where(place < 16, 16 * quad + place, place - 32 - 16 * quad)


def edge_shift(quad):
    shift = jnp.where(quad == 0, EDGE_SHIFT[0], EDGE_SHIFT[1])
    return jnp.where(quad == 2, EDGE_SHIFT[2], jnp.where(quad == 3, EDGE_SHIFT[3], shift))


def lent(device, quad):
    return ((quad == 3) & (device >= 1)) | ((quad == 2) & ((device == 16) | (device == 17)))


def dot(a, b):
    return jnp.dot(a, b, preferred_element_type=jnp.float32)


def kernel(
    kgrid_h, orb, stick_h, fx_h, fym_h, fye_h, fz_h, bz_h, bym_h, bye_h, bx_h,
    out,
    kgrid, own, stick, fx, fym, fye, fz, bz, bym, bye, bx,
    wx, rec, flat_a, flat_b, stage, weights, mask,
    send1, recv1, send2, recv2, later1, got1, later2, got2,
    load_sem, shift_send, shift_recv, a_send, a_recv, b_send, b_recv,
):
    pool = lax.axis_index("pool")
    me = lax.axis_index("fft")
    after = lax.rem(pool + 1, POOL)
    before = lax.rem(pool + POOL - 1, POOL)
    mesh_id = pl.DeviceIdType.MESH

    barrier = pltpu.get_barrier_semaphore()
    pl.semaphore_signal(barrier, inc=1, device_id=(before, me), device_id_type=mesh_id)

    def greet(k, carry):
        peer = lax.rem(me + k, FFT)
        pl.semaphore_signal(barrier, inc=1, device_id=(pool, peer), device_id_type=mesh_id)
        return carry

    lax.fori_loop(1, FFT, greet, 0)
    pairs = (
        (stick_h, stick), (kgrid_h, kgrid), (orb, own), (fx_h, fx), (bx_h, bx), (fym_h, fym),
        (fye_h, fye), (fz_h, fz), (bz_h, bz), (bym_h, bym), (bye_h, bye),
    )
    loads = [pltpu.make_async_copy(far, near, load_sem.at[i]) for i, (far, near) in enumerate(pairs)]
    for load in loads:
        load.start()
    pl.semaphore_wait(barrier, FFT)

    def shift(z):
        return pltpu.make_async_remote_copy(
            src_ref=orb.at[z], dst_ref=rec.at[z],
            send_sem=shift_send.at[z], recv_sem=shift_recv.at[z],
            device_id=(after, me), device_id_type=mesh_id,
        )

    for z in range(PLANES):
        shift(z).start()
    for load in loads:
        load.wait()

    row16 = lax.broadcasted_iota(jnp.int32, (16, LANES), 0)
    near_row = me * (ROWS - 1) + row16
    near_row = jnp.where(near_row < 64, near_row, near_row + 32)
    near_row = jnp.where(row16 < ROWS - 1, near_row, 64 + me)
    edge_row = me + edge_shift(row16 - 8)
    edge_row = jnp.where(edge_row < 0, edge_row + NG, edge_row)
    own_ky = jnp.where(row16 < ROWS, near_row, jnp.where((row16 >= 8) & (row16 < 8 + QUADS), edge_row, -7))
    rank = lax.broadcasted_iota(jnp.int32, (2 * LANES, LANES), 0)
    every_kx = signed_kx(jnp.where(rank < LANES, rank // 32, QUADS), lax.rem(rank, 32))
    every_kx = jnp.where(every_kx < 0, every_kx + NG, every_kx)

    def count(i, total):
        hits_y, hits_x = [], []
        for u in range(5):
            slots = stick[pl.ds(5 * i + u, 1), :]
            row = slots // NG
            ky = jnp.where(slots >= 0, row, -9)
            kx = slots - row * NG
            hits_y.append(jnp.where(own_ky == ky, 1.0, 0.0))
            hits_x.append(jnp.where(every_kx == kx, 1.0, 0.0))
        hit_y = jnp.concatenate(hits_y, axis=1).astype(jnp.bfloat16)
        hit_x = jnp.concatenate(hits_x, axis=1).astype(jnp.bfloat16)
        return total + lax.dot_general(hit_y, hit_x, (((1,), (1,)), ((), ())), preferred_element_type=jnp.float32)

    mask[...] = lax.fori_loop(0, STICK_ROWS // 5, count, jnp.zeros((16, 2 * LANES), jnp.float32))

    pools = lax.broadcasted_iota(jnp.int32, (3, POOL), 1)
    moved = jnp.where(pools == pool, kgrid[...], 0) - jnp.where(pools == before, kgrid[...], 0)
    q = jnp.sum(moved.astype(jnp.float32), axis=1, keepdims=True) / KMESH
    lane = lax.broadcasted_iota(jnp.int32, (NG, LANES), 1)
    freq_z = signed(lax.broadcasted_iota(jnp.int32, (NG, LANES), 0))
    wave_z = freq_z.astype(jnp.float32) + q[2:3]
    cell = SPACING_BOHR * NG
    quad = lax.broadcasted_iota(jnp.int32, (1, LANES), 1) // 32
    outer_held = jnp.zeros((1, LANES), jnp.float32)
    for e in range(QUADS):
        outer_held = jnp.where(quad == e, mask[pl.ds(8 + e, 1), pl.ds(LANES, LANES)], outer_held)
    outer_x = signed_kx(QUADS, lax.rem(lane, 32))
    outer_y = me + edge_shift(lane // 32)
    for r in range(GROUPS):
        if r < ROWS - 1:
            near = me * (ROWS - 1) + r
            freq_x = signed_kx(lane // 32, lax.rem(lane, 32))
            freq_y = jnp.full((NG, LANES), signed(jnp.where(near < 64, near, near + 32)), jnp.int32)
            held = mask[pl.ds(r, 1), pl.ds(0, LANES)]
        elif r < ROWS:
            freq_x = jnp.where(lent(me, lane // 32), outer_x, signed_kx(lane // 32, lax.rem(lane, 32)))
            freq_y = jnp.where(lent(me, lane // 32), outer_y, signed(64 + me))
            held = jnp.where(lent(me, quad), outer_held, mask[pl.ds(r, 1), pl.ds(0, LANES)])
        else:
            freq_x, freq_y = outer_x, outer_y
            held = jnp.where(quad < 2, outer_held, 0.0)
        inside = freq_x * freq_x + freq_y * freq_y + freq_z * freq_z <= (NG // 2) * (NG // 2)
        wave_x = freq_x.astype(jnp.float32) + q[0:1]
        wave_y = freq_y.astype(jnp.float32) + q[1:2]
        square = wave_z * wave_z + (wave_x * wave_x + wave_y * wave_y)
        exponent = math.pi * math.pi * square / (cell * cell * SCREENING * SCREENING)
        weight = cell * cell / math.pi * (1.0 - jnp.exp(-exponent)) / square / float(NG) ** 3
        weights[:, pl.ds(LANES * r, LANES)] = jnp.where(inside & (held > 0.5), weight, 0.0)

    wx[...] = jnp.zeros_like(wx)
    for p in range(2):
        wx[pl.ds(256 * p, NG), :] = fx[pl.ds(NG * p, NG), :]

    lane_quad = lax.broadcasted_iota(jnp.int32, (2 * NG, LANES), 1) // 32

    small_lane = lax.broadcasted_iota(jnp.int32, (FFT, LANES), 1)
    small_lent = lent(lax.broadcasted_iota(jnp.int32, (FFT, LANES), 0), small_lane // 32)

    def joined(real, imaginary):
        return jnp.where(small_lane < HALF, real, pltpu.roll(imaginary, HALF, axis=1))

    def partner(code):
        bits = [(lax.rem(me // (1 << i), 2), lax.rem(code // (1 << i), 2)) for i in range(5)]
        return sum((1 << i) * (mine + other - 2 * mine * other) for i, (mine, other) in enumerate(bits))

    def block_to(peer, send, recv, send_sem, recv_sem):
        return pltpu.make_async_remote_copy(
            src_ref=send.at[peer], dst_ref=recv.at[me],
            send_sem=send_sem, recv_sem=recv_sem,
            device_id=(pool, peer), device_id_type=mesh_id,
        )

    def post(rows, send, recv, send_sem, recv_sem):
        rows = slice(rows[0], rows[0] + rows[1])
        send[...] = stage[...].reshape(FFT, PITCH, LANES)[:, rows].astype(jnp.bfloat16)

        def start(k, carry):
            block_to(partner(FFT - k), send, recv, send_sem, recv_sem).start()
            return carry

        lax.fori_loop(1, FFT, start, 0)
        recv[me] = send[me]

    def others(send, recv, send_sem, recv_sem):
        part = pl.ds(0, OTHERS)
        return pltpu.make_async_remote_copy(
            src_ref=send.at[part], dst_ref=recv.at[part], send_sem=send_sem, recv_sem=recv_sem,
            device_id=(after, me), device_id_type=mesh_id,
        )

    def collect(rows, send, recv, send_sem, recv_sem):
        others(send, recv, send_sem, recv_sem).wait_recv()

        def spread(d, carry):
            start = pl.multiple_of(d * PITCH + rows[0], 8)
            stage[pl.ds(start, rows[1]), :] = recv[d].astype(jnp.float32)
            return carry

        lax.fori_loop(0, FFT, spread, 0, unroll=4)

    out_legs = ((send1, recv1, a_send.at[0], a_recv.at[0]), (later1, got1, a_send.at[1], a_recv.at[1]))
    back_legs = ((send2, recv2, b_send.at[0], b_recv.at[0]), (later2, got2, b_send.at[1], b_recv.at[1]))

    def halves(source, t):
        return [source[pl.ds(2 * t + p, DEEP, stride=2 * TILES), :] for p in range(2)]

    def forward(z, carry):
        flat_a[...] = own[z].astype(jnp.float32)
        shift(z).wait_recv()
        flat_b[...] = rec[z].astype(jnp.float32)
        den_re, den_im = [], []
        for t in range(TILES):
            own_re, own_im = halves(flat_a, t)
            rec_re, rec_im = halves(flat_b, t)
            den_re.append(rec_re * own_re + rec_im * own_im)
            den_im.append(rec_re * own_im - rec_im * own_re)
        runs = []
        for b in range(FOLD):
            parts = [jnp.concatenate(den[b : b + 2], axis=1) for den in (den_re, den_im)]
            if b > 0:
                parts = [pltpu.roll(part, 256 - 32 * b, axis=1) for part in parts]
            runs.append(jnp.concatenate(parts, axis=1))
        along = dot(jnp.concatenate(runs, axis=0).astype(jnp.bfloat16), wx[...])
        planes = [along[:, LANES * k : LANES * (k + 1)] for k in range(4)]
        made = dot(fym[...], jnp.concatenate(planes[:2], axis=0).astype(jnp.bfloat16))
        side = jnp.concatenate(planes[2:], axis=0)
        quads = [jnp.where(lane_quad == e, side, 0.0).astype(jnp.bfloat16) for e in range(QUADS)]
        edge = dot(fye[...], jnp.concatenate(quads, axis=0))
        edges = [edge[p * FFT : (p + 1) * FFT] for p in range(2)]
        for r in range(ROWS):
            for p in range(2):
                piece = made[(2 * r + p) * FFT : (2 * r + p + 1) * FFT]
                if r == ROWS - 1:
                    piece = jnp.where(small_lent, edges[p], piece)
                stage[pl.ds(SHARE * z + 2 * r + p, FFT, stride=PITCH), :] = piece
        stage[pl.ds(SHARE * z + 2 * ROWS, FFT, stride=PITCH), :] = joined(*edges)
        return carry

    lax.fori_loop(0, 3, forward, 0)

    @pl.when((pool < LATE) & (pool != 1))
    def _():
        post(OUT_ROWS[0], *out_legs[0])

    lax.fori_loop(3, PLANES, forward, 0)

    @pl.when((pool >= LATE) | (pool == 1))
    def _():
        post(OUT_ROWS[0], *out_legs[0])

    post(OUT_ROWS[1], *out_legs[1])

    for step in range(2):
        collect(OUT_ROWS[step], *out_legs[step])
    for first in range(0, GROUPS, 2):
        fields = []
        for r in (first, first + 1):
            if r < ROWS:
                runs = [stage[pl.ds(SHARE * z + 2 * r + p, FFT, stride=PITCH), :] for z in range(PLANES) for p in range(2)]
            else:
                both = [stage[pl.ds(SHARE * z + 2 * ROWS, FFT, stride=PITCH), :] for z in range(PLANES)]
                runs = [part for row in both for part in (row, pltpu.roll(row, HALF, axis=1))]
            fields.append(jnp.concatenate(runs, axis=0))
        spectrum = dot(fz[...], jnp.concatenate(fields, axis=1).astype(jnp.bfloat16))
        weight = weights[:, pl.ds(LANES * first, 2 * LANES)]
        scaled = jnp.concatenate([spectrum[:NG] * weight, spectrum[NG:] * weight], axis=0).astype(jnp.bfloat16)
        returned = dot(bz[...], scaled)
        for r in (first, first + 1):
            part = returned[:, LANES * (r - first) : LANES * (r - first + 1)]
            for z in range(PLANES):
                pair = [part[FFT * (2 * z + p) : FFT * (2 * z + p + 1)] for p in range(2)]
                if r < ROWS:
                    for p in range(2):
                        stage[pl.ds(SHARE * z + 2 * r + p, FFT, stride=PITCH), :] = pair[p]
                else:
                    stage[pl.ds(SHARE * z + 2 * ROWS, FFT, stride=PITCH), :] = joined(*pair)

    post(BACK_ROWS[0], *back_legs[0])
    post(BACK_ROWS[1], *back_legs[1])

    def inverse(z, carry):
        flat_b[...] = rec[z].astype(jnp.float32)
        runs = [stage[pl.ds(SHARE * z + i, FFT, stride=PITCH), :] for i in range(SHARE)]
        half_row = (runs[2 * ROWS], pltpu.roll(runs[2 * ROWS], HALF, axis=1))
        last = runs[2 * ROWS - 2 : 2 * ROWS]
        kept = [jnp.where(small_lent, 0.0, row) for row in last]
        main = jnp.concatenate(runs[: 2 * ROWS - 2] + kept, axis=0)
        edge = [jnp.where(small_lane < HALF, half_row[p], jnp.where(small_lent, last[p], 0.0)) for p in range(2)]
        edge = jnp.concatenate(edge, axis=0)
        quads = lane_quad[: 2 * FFT]
        edges = jnp.concatenate([jnp.where(quads == e, edge, 0.0) for e in range(QUADS)], axis=0)
        columns = [dot(bym[...], main.astype(jnp.bfloat16)), dot(bye[...], edges.astype(jnp.bfloat16))]
        parts = [column[NG * p : NG * (p + 1)] for column in columns for p in range(2)]
        along = dot(jnp.concatenate(parts, axis=1).astype(jnp.bfloat16), bx[...])
        shares = []
        for b in range(FOLD):
            windows = [along[DEEP * b : DEEP * (b + 1), 256 * p : 256 * (p + 1)] for p in range(2)]
            if b > 0:
                windows = [pltpu.roll(window, 32 * b, axis=1) for window in windows]
            shares.append(jnp.concatenate(windows, axis=1))
        for t in range(TILES):
            field = []
            for p in range(2):
                low, high = 256 * p, 256 * p + 128
                if t == 0:
                    field.append(shares[0][:, low:high])
                elif t == FOLD:
                    field.append(shares[FOLD - 1][:, high : high + 128])
                else:
                    field.append(shares[t - 1][:, high : high + 128] + shares[t][:, low:high])
            rec_re, rec_im = halves(flat_b, t)
            flat_a[pl.ds(2 * t, DEEP, stride=2 * TILES), :] = rec_im * field[1] - rec_re * field[0]
            flat_a[pl.ds(2 * t + 1, DEEP, stride=2 * TILES), :] = -(rec_re * field[1] + rec_im * field[0])
        out[z] = flat_a[...].astype(jnp.bfloat16)
        return carry

    collect(BACK_ROWS[0], *back_legs[0])
    lax.fori_loop(0, 3, inverse, 0)
    collect(BACK_ROWS[1], *back_legs[1])
    lax.fori_loop(3, PLANES, inverse, 0)

    for z in range(PLANES):
        shift(z).wait_send()
    for leg in out_legs + back_legs:
        others(*leg).wait_send()


def local(orbitals, stick_map, kpoint_grid):
    orb = orbitals.reshape(2, PLANES, TILES * DEEP, LANES).transpose(1, 2, 0, 3).reshape(PLANES, RAW, LANES)
    stick = stick_map.reshape(STICK_ROWS, LANES)
    constants = tables()
    orb, stick, kgrid_t = (pltpu.with_memory_space_constraint(a, pltpu.HBM) for a in (orb, stick, kpoint_grid.T))
    constants = [pltpu.with_memory_space_constraint(c, pltpu.HBM) for c in constants]
    far = pl.BlockSpec(memory_space=pltpu.HBM)
    bf16, f32 = jnp.bfloat16, jnp.float32
    result = pl.pallas_call(
        kernel,
        name="exchange_step",
        out_shape=jax.ShapeDtypeStruct(orb.shape, bf16),
        in_specs=[far] * (3 + len(constants)),
        out_specs=pl.BlockSpec(memory_space=pltpu.VMEM),
        scratch_shapes=[
            pltpu.VMEM((3, POOL), jnp.int32),
            pltpu.VMEM(orb.shape, bf16),
            pltpu.VMEM(stick.shape, jnp.int32),
        ]
        + [pltpu.VMEM(t.shape, bf16) for t in constants]
        + [
            pltpu.VMEM((512, 512), bf16),
            pltpu.VMEM(orb.shape, bf16),
            pltpu.VMEM((RAW, LANES), f32),
            pltpu.VMEM((RAW, LANES), f32),
            pltpu.VMEM((FFT * PITCH, LANES), f32),
            pltpu.VMEM((NG, GROUPS * LANES), f32),
            pltpu.VMEM((16, 2 * LANES), f32),
        ]
        + [pltpu.VMEM((FFT, rows[k][1], LANES), bf16) for k in range(2) for rows in (OUT_ROWS, OUT_ROWS, BACK_ROWS, BACK_ROWS)]
        + [
            pltpu.SemaphoreType.DMA((3 + len(constants),)),
            pltpu.SemaphoreType.DMA((PLANES,)),
            pltpu.SemaphoreType.DMA((PLANES,)),
        ]
        + [pltpu.SemaphoreType.DMA((2,))] * 4,
        compiler_params=pltpu.CompilerParams(
            collective_id=0, has_side_effects=True, vmem_limit_bytes=48 * 1024 * 1024
        ),
    )(kgrid_t, orb, stick, *constants)
    result = result.reshape(PLANES, TILES * DEEP, 2, LANES).transpose(2, 0, 1, 3)
    return result.reshape(1, 2, 1, PLANES, NG * NG)


def solution(mesh):
    return jax.shard_map(
        local,
        mesh=mesh,
        in_specs=(P("pool", None, None, "fft", None), P(), P()),
        out_specs=P("pool", None, None, "fft", None),
        check_vma=False,
    )
```
